32 devices in a mesh: grp: 2 (over x), row: 16 (over z, y, core).
Axes of the slice: x: 2, y: 2, z: 4, core: 2. Of those that a mesh axis runs over, the one named last changes fastest.
Arguments:
- alignment: bfloat16 [128, 128, 256], P(('grp', 'row')), parts along dimension 0, may hold values from -6 to 6
- seq_flags: int32 [128], P(('grp', 'row')), parts along dimension 0, may hold values 0 or 1
- crop_flags: int32 [256], P('grp'), parts along dimension 0, may hold values 0 or 1
- norm_gain: float32 [256], replicated, may hold values from 0.5 to 1.5
- norm_bias: float32 [256], replicated, may hold values from -3 to 3
- left_weight: bfloat16 [256, 32], replicated, may hold values from -0.375 to 0.375
- left_bias: float32 [32], replicated, may hold values from -3 to 3
- right_weight: bfloat16 [256, 32], replicated, may hold values from -0.375 to 0.375
- right_bias: float32 [32], replicated, may hold values from -3 to 3
- out_weight: bfloat16 [1024, 128], replicated, may hold values from -0.1875 to 0.1875
- out_bias: float32 [128], replicated, may hold values from -3 to 3
Outputs:
- pair_update: bfloat16 [256, 128, 128], P(('grp', 'row')), parts along dimension 0
The draws below stay inside these ranges and needn't reach their ends.
There are 2 independent parts, one for each index of `grp`. The reference program is written for one: setup_inputs(seed, part) draws one part's arguments, and reference() takes and returns one part's arrays. A program takes and returns all parts, laid end to end along the dimension named above; an argument that names none is the same for every part. Nothing has to cross between parts.
All inputs are finite; a program needn't handle non-finite values. No bound on the sum of `seq_flags` on one device may be relied on, other than what follows from the above.
Results may differ from the reference program's by a relative error of at most 0.004.
Values may be sent and summed in bfloat16 or wider, within the bound.
No kernel may reach another device: no remote copies, remote signals or barrier semaphores. Data moves between devices by JAX's collectives and lax.ppermute only.
A program may use at most 128 MiB of HBM per device.

```python
import jax
import jax.numpy as jnp
from jax import lax

C_M = 256
C = 32
P_SIZE = 128
RES_DEV = 8
S = 64
R = 128


def touch_ends(drawn, own_key, smallest, largest):
    index_at = [jax.random.randint(jax.random.fold_in(own_key, axis), (), 0, length) for axis, length in enumerate(drawn.shape)]
    main_axis = drawn.shape.index(max(drawn.shape))
    neighbour = index_at[:main_axis] + [(index_at[main_axis] + 1) % drawn.shape[main_axis]] + index_at[main_axis + 1:]
    return drawn.at[tuple(index_at)].set(smallest).at[tuple(neighbour)].set(largest)


def steps_of(rng, dims, split, smallest, high):
    gain, own = 1.0, jax.random.fold_in(rng, 6)
    for position, shards_of in split:
        draws = jnp.exp(jax.random.uniform(jax.random.fold_in(own, position), (shards_of,), jnp.float32, smallest / len(split), high / len(split)))
        gain = gain * jnp.repeat(draws, dims[position] // shards_of).reshape([-1 if axis == position else 1 for axis in range(len(dims))])
    return gain


def centred(own_key, dims, width, most, pieces=(), kind=jnp.bfloat16):
    values = jax.random.normal(own_key, dims, jnp.float32) * width
    if len(pieces) > 0:
        values = steps_of(own_key, dims, pieces, -0.22, 0.18) * values
    return jnp.clip(values, min=-most, max=most).astype(kind)


def setup_inputs(seed: int = 0, part: int = 0) -> dict:
    splits = jax.random.split(jax.random.key(seed), 12)
    part_splits = jax.random.split(jax.random.fold_in(splits[11], part), 12)
    alignment = centred(part_splits[0], (S, R, C_M), 1.0, 6.0, ((0, 16),))
    seq_flags = touch_ends((jax.random.randint(part_splits[1], (S,), 0, 4) < 3).astype(jnp.int32), jax.random.fold_in(part_splits[1], 1), 0, 1)
    crop_flags = touch_ends((jax.random.randint(part_splits[2], (R,), 0, 8) < 7).astype(jnp.int32), jax.random.fold_in(part_splits[2], 1), 0, 1)
    norm_gain = jnp.clip(1.0 + 0.1 * jax.random.normal(splits[3], (C_M,), jnp.float32), 0.5, 1.5)
    norm_bias = centred(splits[4], (C_M,), 0.5, 3.0, (), jnp.float32)
    left_weight = centred(splits[5], (C_M, C), C_M ** -0.5, 0.375)
    left_bias = centred(splits[6], (C,), 0.5, 3.0, (), jnp.float32)
    right_weight = centred(splits[7], (C_M, C), C_M ** -0.5, 0.375)
    right_bias = centred(splits[8], (C,), 0.5, 3.0, (), jnp.float32)
    out_weight = centred(splits[9], (C * C, P_SIZE), (C * C) ** -0.5, 0.1875)
    out_bias = centred(splits[10], (P_SIZE,), 0.5, 3.0, (), jnp.float32)
    return dict(alignment=alignment, seq_flags=seq_flags, crop_flags=crop_flags, norm_gain=norm_gain, norm_bias=norm_bias, left_weight=left_weight, left_bias=left_bias, right_weight=right_weight, right_bias=right_bias, out_weight=out_weight, out_bias=out_bias)


def normalize(values, norm_gain, norm_bias):
    values = values.astype(jnp.float32)
    average = lax.optimization_barrier(jnp.mean(values, axis=-1, keepdims=True))
    variance = lax.optimization_barrier(jnp.mean((values - average) ** 2, axis=-1, keepdims=True))
    return (values - average) * lax.rsqrt(variance + 1e-05) * norm_gain + norm_bias

def project(normed, weight, bias, scaling):
    product = jnp.einsum('src,cd->srd', normed, weight.astype(jnp.float32), precision=lax.Precision.HIGHEST)
    return ((product + bias) * scaling).astype(jnp.bfloat16)

def reference(alignment, seq_flags, crop_flags, norm_gain, norm_bias, left_weight, left_bias, right_weight, right_bias, out_weight, out_bias):
    normed = normalize(alignment, norm_gain, norm_bias)
    crop_float = crop_flags.astype(jnp.float32)
    scaling = seq_flags.astype(jnp.float32)[:, None, None] * crop_float[None, :, None]
    left = project(normed, left_weight, left_bias, scaling)
    right = project(normed, right_weight, right_bias, scaling)
    live_count = jnp.sum(seq_flags.astype(jnp.float32))
    right_flat = right.reshape(S, R * C)

    def row_block(block_index):
        offset = (block_index * RES_DEV).astype(jnp.int32)
        left_block = lax.dynamic_slice_in_dim(left, offset, RES_DEV, 1).reshape(S, RES_DEV * C)
        sums = lax.dot_general(left_block, right_flat, (((0,), (0,)), ((), ())), preferred_element_type=jnp.float32)
        outer_sum = sums.reshape(RES_DEV, C, R, C).transpose(0, 2, 1, 3).reshape(RES_DEV * R, C * C).astype(jnp.bfloat16)
        projected = jnp.dot(outer_sum, out_weight, preferred_element_type=jnp.float32).reshape(RES_DEV, R, P_SIZE)
        crop_rows = lax.dynamic_slice_in_dim(crop_float, offset, RES_DEV, 0)
        divisor = jnp.maximum(live_count * crop_rows[:, None] * crop_float[None, :], 1.0)
        return (projected / divisor[:, :, None] + out_bias).astype(jnp.bfloat16)
    blocks = lax.map(row_block, jnp.arange(R // RES_DEV, dtype=jnp.int32))
    return blocks.reshape(R, R, P_SIZE)
```

```python
import functools

import jax
import jax.numpy as jnp
from jax import lax
from jax.experimental import pallas as pl
from jax.experimental.pallas import tpu as pltpu
from jax.sharding import PartitionSpec as P

F32 = jnp.float32
BF16 = jnp.bfloat16
FLAG_ROWS = 8


def _iota(shape, dim):
    return lax.broadcasted_iota(jnp.int32, shape, dim)


def _dot_t(lhs, rhs, **kw):
    return lax.dot_general(
        lhs, rhs, (((1,), (1,)), ((), ())), preferred_element_type=F32, **kw
    )


def _column(row):
    length = row.shape[1]
    square = (length, length)
    picked = jnp.where(
        _iota(square, 0) == _iota(square, 1), jnp.broadcast_to(row, square), 0.0
    )
    return jnp.sum(picked, axis=1, keepdims=True)


def _vmem(n):
    return [pl.BlockSpec(memory_space=pltpu.VMEM)] * n


def _project_kernel(
    x_ref, flags_ref, crop_ref, gain_ref, shift_ref, wl_ref, wr_ref, lb_ref, rb_ref, out_ref
):
    seqs, residues, _ = x_ref.shape
    channels = wl_ref.shape[0]
    pair = 2 * seqs
    lanes = pair * channels
    first = (lax.axis_index("row") % 2) * seqs
    spread = _iota((lanes, channels), 0)
    which = _iota((lanes, channels), 1)
    pick_r = jnp.where(spread // pair == which, 1.0, 0.0)
    pick_l = jnp.where(spread % channels == which, 1.0, 0.0)
    exact = dict(precision=lax.Precision.HIGHEST)
    wr_rep = jnp.dot(pick_r.astype(BF16), wr_ref[...], preferred_element_type=F32).astype(BF16)
    wl_rep = jnp.concatenate([wl_ref[...]] * pair, axis=0)
    rb_rep = _dot_t(jnp.broadcast_to(rb_ref[...], (8, channels)), pick_r, **exact)[0:1]
    lb_rep = _dot_t(jnp.broadcast_to(lb_ref[...], (8, channels)), pick_l, **exact)[0:1]
    crop = _column(crop_ref[...].astype(F32))
    lane = _iota((1, lanes), 1)
    seq_r = lane % pair - first
    seq_l = lane // channels - first
    right = jnp.zeros((residues, lanes), F32)
    left = jnp.zeros((residues, lanes), F32)
    flag_r = jnp.zeros((1, lanes), F32)
    flag_l = jnp.zeros((1, lanes), F32)
    flag_row = jnp.zeros((1, lanes), F32)
    for s in range(seqs):
        values = x_ref[s].astype(F32)
        values = values - jnp.mean(values, axis=-1, keepdims=True)
        variance = jnp.mean(values * values, axis=-1, keepdims=True)
        normed = values * lax.rsqrt(variance + 1e-05) * gain_ref[...] + shift_ref[...]
        high = normed.astype(BF16)
        low = (normed - high.astype(F32)).astype(BF16)
        flag = flags_ref[s].astype(F32)
        right = jnp.where(seq_r == s, _dot_t(high, wr_rep) + _dot_t(low, wr_rep), right)
        left = jnp.where(seq_l == s, _dot_t(high, wl_rep) + _dot_t(low, wl_rep), left)
        flag_r = jnp.where(seq_r == s, flag, flag_r)
        flag_l = jnp.where(seq_l == s, flag, flag_l)
        flag_row = jnp.where(lane - first == s, flag, flag_row)
    out_ref[0:residues] = ((right + rb_rep) * (flag_r * crop)).astype(BF16)
    out_ref[residues : 2 * residues] = ((left + lb_rep) * (flag_l * crop)).astype(BF16)
    rows = _iota((2 * FLAG_ROWS, lanes), 0)
    out_ref[2 * residues :] = jnp.where(rows == 0, flag_row, 0.0).astype(BF16)


def _pack_kernel(steps, rows_chip, own_ref, other_ref, *out_refs):
    residues = own_ref.shape[0] // 2 - FLAG_ROWS
    total = rows_chip + FLAG_ROWS
    index = lax.axis_index("row")
    chip, core = index // 2, index % 2
    right = own_ref[0:residues] + other_ref[0:residues]
    flags = own_ref[2 * residues :] + other_ref[2 * residues :]
    for out_ref, (far, near) in zip(out_refs, ((0, 0),) + steps):
        target = chip ^ jnp.where(core == 1, far, near)
        start = pl.multiple_of(residues + target * rows_chip, rows_chip)
        out_ref[0:residues] = right
        slab = own_ref[pl.ds(start, rows_chip)] + other_ref[pl.ds(start, rows_chip)]
        tail = jnp.concatenate([slab.astype(F32), flags.astype(F32)], axis=0)
        out_ref[residues : residues + total] = tail[0:total].astype(BF16)


def _weight_kernel(channels, w_ref, out_ref, wide_ref):
    width = w_ref.shape[1]
    wide_ref[...] = w_ref[...].astype(F32)
    for e in range(channels):
        block = wide_ref[pl.ds(e, channels, stride=channels), :]
        out_ref[:, e * width : (e + 1) * width] = block.astype(BF16)


def _partial(parcels, w_ref, a_ref):
    channels = w_ref.shape[0]
    lanes = parcels[0].shape[1]
    pair = lanes // channels
    width = w_ref.shape[1] // channels
    residues = parcels[0].shape[0] - 2 * pair - FLAG_ROWS
    core = lax.axis_index("row") % 2
    mine = _iota((pair, lanes), 1) // channels == _iota((pair, lanes), 0)
    rows = []
    for ref in parcels:
        slab = ref[residues : residues + 2 * pair].astype(F32)
        slab = jnp.where(core == 1, slab[pair:], slab[:pair])
        for i in range(pair):
            rows.append(jnp.where(mine, jnp.broadcast_to(slab[i : i + 1], (pair, lanes)), 0.0))
    spread = jnp.concatenate(rows, axis=0).astype(BF16)
    for e in range(0, channels, 2):
        block = w_ref[:, e * width : (e + 2) * width]
        product = jnp.dot(
            spread, jnp.concatenate([block] * pair, axis=0), preferred_element_type=F32
        )
        for n in range(len(parcels)):
            for i in range(pair):
                at = (n * pair + i) * pair
                both = jnp.concatenate(
                    [product[at : at + pair, :width], product[at : at + pair, width:]], axis=0
                )
                a_ref[
                    n * lanes + e * pair : n * lanes + (e + 2) * pair,
                    i * width : (i + 1) * width,
                ] = both.astype(BF16)
    total = None
    for n, ref in enumerate(parcels):
        part = jnp.dot(
            ref[0:residues], a_ref[n * lanes : (n + 1) * lanes], preferred_element_type=F32
        )
        total = part if total is None else total + part
    return total


def _live(parcels):
    total = None
    for ref in parcels:
        rows = ref.shape[0]
        part = ref[rows - 2 * FLAG_ROWS :].astype(F32)[FLAG_ROWS:]
        total = part if total is None else total + part
    return total


def _first_kernel(count, w_ref, *refs):
    parcels, (sum_ref, live_ref, a_ref) = refs[:count], refs[count:]
    sum_ref[...] = _partial(parcels, w_ref, a_ref)
    live_ref[...] = _live(parcels)


def _last_kernel(count, w_ref, sum_in, live_in, crop_ref, bias_ref, *refs):
    parcels, (out_ref, a_ref) = refs[:count], refs[count:]
    rows_here, _, width = out_ref.shape
    projected = sum_in[...] + _partial(parcels, w_ref, a_ref)
    live = jnp.sum(live_in[...] + _live(parcels))
    crop = crop_ref[...].astype(F32)
    column = _column(crop)
    first = lax.axis_index("row") * rows_here
    lane = _iota(crop.shape, 1)
    for i in range(rows_here):
        crop_i = jnp.sum(jnp.where(lane == first + i, crop, 0.0))
        divisor = jnp.maximum(live * crop_i * column, 1.0)
        tile = projected[:, i * width : (i + 1) * width] / divisor + bias_ref[...]
        out_ref[i] = tile.astype(BF16)


def per_device(
    alignment,
    seq_flags,
    crop_flags,
    norm_gain,
    norm_bias,
    left_weight,
    left_bias,
    right_weight,
    right_bias,
    out_weight,
    out_bias,
):
    seqs, residues, _ = alignment.shape
    channels = left_weight.shape[1]
    width = out_weight.shape[1]
    devices = lax.axis_size("row")
    rows_here = residues // devices
    rows_chip = 2 * rows_here
    chips = devices // 2
    lanes = 2 * seqs * channels
    steps = tuple((k, (k + 1) % chips) for k in range(1, chips, 2))
    cores = [(d, d ^ 1) for d in range(devices)]
    crop = crop_flags.reshape(1, residues)
    limit = pltpu.CompilerParams(vmem_limit_bytes=48 * 1024 * 1024)

    projected = pl.pallas_call(
        _project_kernel,
        out_shape=jax.ShapeDtypeStruct((2 * residues + 2 * FLAG_ROWS, lanes), BF16),
        in_specs=_vmem(1) + [pl.BlockSpec(memory_space=pltpu.SMEM)] + _vmem(7),
        out_specs=_vmem(1)[0],
        compiler_params=limit,
        name="project",
    )(
        alignment,
        seq_flags,
        crop,
        norm_gain.reshape(1, -1),
        norm_bias.reshape(1, -1),
        left_weight.T,
        right_weight.T,
        left_bias.reshape(1, -1),
        right_bias.reshape(1, -1),
    )
    other = lax.ppermute(projected, "row", cores)
    parcel = jax.ShapeDtypeStruct((residues + rows_chip + FLAG_ROWS, lanes), BF16)
    own, *parcels = pl.pallas_call(
        functools.partial(_pack_kernel, steps, rows_chip),
        out_shape=[parcel] * (1 + len(steps)),
        in_specs=_vmem(2),
        out_specs=_vmem(1 + len(steps)),
        compiler_params=limit,
        name="pack",
    )(projected, other)
    received = []
    for (far, near), piece in zip(steps, parcels):
        pairs = [(2 * q + 1, 2 * (q ^ far) + 1) for q in range(chips)]
        if near:
            pairs += [(2 * q, 2 * (q ^ near)) for q in range(chips)]
        received.append(lax.ppermute(piece, "row", pairs))
    handed = [lax.ppermute(piece, "row", cores) for piece in received]

    weight = pl.pallas_call(
        functools.partial(_weight_kernel, channels),
        out_shape=jax.ShapeDtypeStruct((channels, channels * width), BF16),
        in_specs=_vmem(1),
        out_specs=_vmem(1)[0],
        scratch_shapes=[pltpu.VMEM(out_weight.shape, F32)],
        compiler_params=limit,
        name="weight",
    )(out_weight)
    here = [own] + received
    partial_sum, live = pl.pallas_call(
        functools.partial(_first_kernel, len(here)),
        out_shape=[
            jax.ShapeDtypeStruct((residues, rows_here * width), F32),
            jax.ShapeDtypeStruct((FLAG_ROWS, lanes), F32),
        ],
        in_specs=_vmem(1 + len(here)),
        out_specs=_vmem(2),
        scratch_shapes=[pltpu.VMEM((len(here) * lanes, rows_here * width), BF16)],
        compiler_params=limit,
        name="first",
    )(weight, *here)
    return pl.pallas_call(
        functools.partial(_last_kernel, len(handed)),
        out_shape=jax.ShapeDtypeStruct((rows_here, residues, width), BF16),
        in_specs=_vmem(5 + len(handed)),
        out_specs=_vmem(1)[0],
        scratch_shapes=[pltpu.VMEM((len(handed) * lanes, rows_here * width), BF16)],
        compiler_params=limit,
        name="last",
    )(weight, partial_sum, live, crop, out_bias.reshape(1, -1), *handed)


def solution(mesh):
    return jax.shard_map(
        per_device,
        mesh=mesh,
        in_specs=(
            P(("grp", "row"), None, None),
            P(("grp", "row")),
            P("grp"),
            P(),
            P(),
            P(),
            P(),
            P(),
            P(),
            P(),
            P(),
        ),
        out_specs=P(("grp", "row"), None, None),
        check_vma=False,
    )
```

```python
import functools

import jax
import jax.numpy as jnp
from jax import lax
from jax.experimental import pallas as pl
from jax.experimental.pallas import tpu as pltpu
from jax.sharding import PartitionSpec as P


F32 = jnp.float32
BF16 = jnp.bfloat16
FLAG_ROWS = 8


def _iota(shape, dim):
    return lax.broadcasted_iota(jnp.int32, shape, dim)


def _column(row):
    length = row.shape[1]
    square = (length, length)
    picked = jnp.where(
        _iota(square, 0) == _iota(square, 1), jnp.broadcast_to(row, square), 0.0
    )
    return jnp.sum(picked, axis=1, keepdims=True)


def _stay(array):
    return pltpu.with_memory_space_constraint(array, pltpu.HBM)


def _vmem(n):
    return [pl.BlockSpec(memory_space=pltpu.VMEM)] * n


def _project_kernel(
    x_hbm,
    flags_hbm,
    crop_hbm,
    gain_hbm,
    shift_hbm,
    wl_hbm,
    wr_hbm,
    lb_hbm,
    rb_hbm,
    out_ref,
    x_ref,
    flags_ref,
    crop_ref,
    gain_ref,
    shift_ref,
    wl_ref,
    wr_ref,
    lb_ref,
    rb_ref,
    x_sems,
    sems,
):
    seqs, residues, _ = x_ref.shape
    channels = wl_ref.shape[0]
    small = [
        pltpu.make_async_copy(src, dst, sems.at[n])
        for n, (src, dst) in enumerate(
            [
                (wr_hbm, wr_ref),
                (wl_hbm, wl_ref),
                (gain_hbm, gain_ref),
                (shift_hbm, shift_ref),
                (crop_hbm, crop_ref),
                (flags_hbm, flags_ref),
                (lb_hbm, lb_ref),
                (rb_hbm, rb_ref),
            ]
        )
    ]
    loads = [
        pltpu.make_async_copy(x_hbm.at[s], x_ref.at[s], x_sems.at[s]) for s in range(seqs)
    ]
    for copy in loads + small:
        copy.start()
    pair = 2 * seqs
    lanes = pair * channels
    first = (lax.axis_index("row") % 2) * seqs
    which = _iota((channels, lanes), 0)
    spread = _iota((channels, lanes), 1)
    pick_r = jnp.where(spread // pair == which, 1.0, 0.0)
    pick_l = jnp.where(spread % channels == which, 1.0, 0.0)
    exact = dict(precision=lax.Precision.HIGHEST, preferred_element_type=F32)
    lane = _iota((1, lanes), 1)
    seq_r = lane % pair - first
    seq_l = lane // channels - first
    for copy in small:
        copy.wait()
    turned = (((0,), (0,)), ((), ()))
    wr_rep = lax.dot_general(
        wr_ref[...], pick_r.astype(BF16), turned, preferred_element_type=F32
    ).astype(BF16)
    wl_rep = lax.dot_general(
        wl_ref[...], pick_l.astype(BF16), turned, preferred_element_type=F32
    ).astype(BF16)
    rb_rep = jnp.dot(jnp.broadcast_to(rb_ref[...], (8, channels)), pick_r, **exact)[0:1]
    lb_rep = jnp.dot(jnp.broadcast_to(lb_ref[...], (8, channels)), pick_l, **exact)[0:1]
    crop = _column(crop_ref[...].astype(F32))
    right = jnp.zeros((residues, lanes), F32)
    left = jnp.zeros((residues, lanes), F32)
    flag_r = jnp.zeros((1, lanes), F32)
    flag_l = jnp.zeros((1, lanes), F32)
    flag_row = jnp.zeros((1, lanes), F32)
    flags = flags_ref[...].astype(F32)
    for s in range(seqs):
        flag = jnp.broadcast_to(flags[:, s : s + 1], (1, lanes))
        flag_r = jnp.where(seq_r == s, flag, flag_r)
        flag_l = jnp.where(seq_l == s, flag, flag_l)
        flag_row = jnp.where(lane - first == s, flag, flag_row)
    for s in range(seqs):
        loads[s].wait()
        values = x_ref[s].astype(F32)
        values = values - jnp.mean(values, axis=-1, keepdims=True)
        variance = jnp.mean(values * values, axis=-1, keepdims=True)
        normed = values * lax.rsqrt(variance + 1e-05) * gain_ref[...] + shift_ref[...]
        high = normed.astype(BF16)
        low = (normed - high.astype(F32)).astype(BF16)
        to_right = jnp.dot(high, wr_rep, preferred_element_type=F32) + jnp.dot(
            low, wr_rep, preferred_element_type=F32
        )
        to_left = jnp.dot(high, wl_rep, preferred_element_type=F32) + jnp.dot(
            low, wl_rep, preferred_element_type=F32
        )
        right = jnp.where(seq_r == s, to_right, right)
        left = jnp.where(seq_l == s, to_left, left)
    out_ref[0:residues] = ((right + rb_rep) * (flag_r * crop)).astype(BF16)
    out_ref[residues : 2 * residues] = ((left + lb_rep) * (flag_l * crop)).astype(BF16)
    rows = _iota((2 * FLAG_ROWS, lanes), 0)
    out_ref[2 * residues :] = jnp.where(rows == 0, flag_row, 0.0).astype(BF16)


def _pack_kernel(steps, rows_chip, own_ref, other_ref, *out_refs):
    residues = own_ref.shape[0] // 2 - FLAG_ROWS
    total = rows_chip + FLAG_ROWS
    index = lax.axis_index("row")
    chip, core = index // 2, index % 2
    right = own_ref[0:residues] + other_ref[0:residues]
    flags = own_ref[2 * residues :] + other_ref[2 * residues :]
    for out_ref, (far, near) in zip(out_refs, ((0, 0),) + steps):
        target = chip ^ jnp.where(core == 1, far, near)
        start = pl.multiple_of(residues + target * rows_chip, rows_chip)
        out_ref[0:residues] = right
        slab = own_ref[pl.ds(start, rows_chip)] + other_ref[pl.ds(start, rows_chip)]
        tail = jnp.concatenate([slab.astype(F32), flags.astype(F32)], axis=0)
        out_ref[residues : residues + total] = tail[0:total].astype(BF16)


def _read(slot, rows):
    if not isinstance(slot, tuple):
        return slot[rows]
    north, south = slot
    return jnp.where(lax.axis_index("row") % 2 == 1, north[rows], south[rows])


def _rows(slot):
    return (slot[0] if isinstance(slot, tuple) else slot).shape


def _partial(slots, w_ref, a_ref):
    channels = w_ref.shape[0]
    height, lanes = _rows(slots[0])
    pair = lanes // channels
    width = w_ref.shape[1] // channels
    residues = height - 2 * pair - FLAG_ROWS
    core = lax.axis_index("row") % 2
    mine = _iota((pair, lanes), 1) // channels == _iota((pair, lanes), 0)
    rows = []
    for slot in slots:
        slab = _read(slot, slice(residues, residues + 2 * pair)).astype(F32)
        slab = jnp.where(core == 1, slab[pair:], slab[:pair])
        for i in range(pair):
            rows.append(jnp.where(mine, jnp.broadcast_to(slab[i : i + 1], (pair, lanes)), 0.0))
    spread = jnp.concatenate(rows, axis=0).astype(BF16)
    for e in range(0, channels, 2):
        block = w_ref[:, e * width : (e + 2) * width]
        product = jnp.dot(
            spread, jnp.concatenate([block] * pair, axis=0), preferred_element_type=F32
        )
        for n in range(len(slots)):
            for i in range(pair):
                at = (n * pair + i) * pair
                both = jnp.concatenate(
                    [product[at : at + pair, :width], product[at : at + pair, width:]], axis=0
                )
                a_ref[
                    n * lanes + e * pair : n * lanes + (e + 2) * pair,
                    i * width : (i + 1) * width,
                ] = both.astype(BF16)
    total = None
    for n, slot in enumerate(slots):
        part = jnp.dot(
            _read(slot, slice(0, residues)),
            a_ref[n * lanes : (n + 1) * lanes],
            preferred_element_type=F32,
        )
        total = part if total is None else total + part
    return total


def _live(slots):
    total = None
    for slot in slots:
        rows = _rows(slot)[0]
        part = _read(slot, slice(rows - 2 * FLAG_ROWS, rows)).astype(F32)[FLAG_ROWS:]
        total = part if total is None else total + part
    return total


def _first_kernel(channels, w_hbm, own_ref, w_ref, sum_ref, live_ref, raw_ref, wide_ref, a_ref, sem):
    copy = pltpu.make_async_copy(w_hbm, raw_ref, sem)
    copy.start()
    copy.wait()
    width = raw_ref.shape[1]
    wide_ref[...] = raw_ref[...].astype(F32)
    for e in range(channels):
        block = wide_ref[pl.ds(e, channels, stride=channels), :]
        w_ref[:, e * width : (e + 1) * width] = block.astype(BF16)
    sum_ref[...] = _partial([own_ref], w_ref, a_ref)
    live_ref[...] = _live([own_ref])


def _more_kernel(count, w_ref, sum_in, live_in, *refs):
    parcels, (sum_ref, live_ref, a_ref) = refs[:count], refs[count:]
    sum_ref[...] = sum_in[...] + _partial(parcels, w_ref, a_ref)
    live_ref[...] = live_in[...] + _live(parcels)


def _last_kernel(
    w_ref,
    sum_in,
    live_in,
    crop_hbm,
    bias_hbm,
    north_ref,
    south_ref,
    out_hbm,
    a_ref,
    crop_ref,
    bias_ref,
    out_ref,
    sems,
    out_sems,
):
    loads = [
        pltpu.make_async_copy(crop_hbm, crop_ref, sems.at[0]),
        pltpu.make_async_copy(bias_hbm, bias_ref, sems.at[1]),
    ]
    for copy in loads:
        copy.start()
    slots = [(north_ref, south_ref)]
    rows_here, _, width = out_ref.shape
    live = jnp.sum(live_in[...] + _live(slots))
    projected = sum_in[...] + _partial(slots, w_ref, a_ref)
    for copy in loads:
        copy.wait()
    crop = crop_ref[...].astype(F32)
    column = _column(crop)
    first = lax.axis_index("row") * rows_here
    lane = _iota(crop.shape, 1)
    stores = []
    for i in range(rows_here):
        crop_i = jnp.sum(jnp.where(lane == first + i, crop, 0.0), axis=1, keepdims=True)
        inverse = 1.0 / jnp.maximum(live * crop_i * column, 1.0)
        tile = projected[:, i * width : (i + 1) * width] * inverse + bias_ref[...]
        out_ref[i] = tile.astype(BF16)
        stores.append(pltpu.make_async_copy(out_ref.at[i], out_hbm.at[i], out_sems.at[i]))
        stores[-1].start()
    for copy in stores:
        copy.wait()


def per_device(
    alignment,
    seq_flags,
    crop_flags,
    norm_gain,
    norm_bias,
    left_weight,
    left_bias,
    right_weight,
    right_bias,
    out_weight,
    out_bias,
):
    seqs, residues, _ = alignment.shape
    channels = left_weight.shape[1]
    width = out_weight.shape[1]
    devices = lax.axis_size("row")
    rows_here = residues // devices
    rows_chip = 2 * rows_here
    chips = devices // 2
    lanes = 2 * seqs * channels
    half, quarter = chips // 2, max(1, chips // 4)
    steps = tuple(
        zip(
            [quarter] + [k for k in range(chips - 1, half, -1) if k != quarter],
            [k for k in range(half, 0, -1) if k != quarter] + [0],
        )
    )
    cores = [(d, d ^ 1) for d in range(devices)]
    crop = crop_flags.reshape(1, residues)
    limit = pltpu.CompilerParams(vmem_limit_bytes=48 * 1024 * 1024)
    anywhere = pl.BlockSpec(memory_space=pltpu.HBM)

    operands = (
        alignment,
        seq_flags.reshape(1, seqs),
        crop,
        norm_gain.reshape(1, -1),
        norm_bias.reshape(1, -1),
        left_weight.T,
        right_weight.T,
        left_bias.reshape(1, -1),
        right_bias.reshape(1, -1),
    )
    projected = pl.pallas_call(
        _project_kernel,
        out_shape=jax.ShapeDtypeStruct((2 * residues + 2 * FLAG_ROWS, lanes), BF16),
        in_specs=[anywhere] * len(operands),
        out_specs=_vmem(1)[0],
        scratch_shapes=[pltpu.VMEM(a.shape, a.dtype) for a in operands]
        + [pltpu.SemaphoreType.DMA((seqs,)), pltpu.SemaphoreType.DMA((len(operands) - 1,))],
        compiler_params=limit,
        name="project",
    )(*map(_stay, operands))
    other = lax.ppermute(projected, "row", cores)
    parcel = jax.ShapeDtypeStruct((residues + rows_chip + FLAG_ROWS, lanes), BF16)
    own, *parcels = pl.pallas_call(
        functools.partial(_pack_kernel, steps, rows_chip),
        out_shape=[parcel] * (1 + len(steps)),
        in_specs=_vmem(2),
        out_specs=_vmem(1 + len(steps)),
        compiler_params=limit,
        name="pack",
    )(projected, other)
    received, handed = [], []
    for (far, near), piece in zip(steps, parcels):
        pairs = [(2 * q + 1, 2 * (q ^ far) + 1) for q in range(chips)]
        back = [(2 * q + 1, 2 * q) for q in range(chips)]
        if near:
            pairs += [(2 * q, 2 * (q ^ near)) for q in range(chips)]
            back += [(2 * q, 2 * q + 1) for q in range(chips)]
        received.append(lax.ppermute(piece, "row", pairs))
        handed.append(lax.ppermute(received[-1], "row", back))

    columns = rows_here * width
    state = [
        jax.ShapeDtypeStruct((residues, columns), F32),
        jax.ShapeDtypeStruct((FLAG_ROWS, lanes), F32),
    ]
    weight, *carry = pl.pallas_call(
        functools.partial(_first_kernel, channels),
        out_shape=[jax.ShapeDtypeStruct((channels, channels * width), BF16)] + state,
        in_specs=[anywhere] + _vmem(1),
        out_specs=_vmem(3),
        scratch_shapes=[
            pltpu.VMEM(out_weight.shape, BF16),
            pltpu.VMEM(out_weight.shape, F32),
            pltpu.VMEM((lanes, columns), BF16),
            pltpu.SemaphoreType.DMA,
        ],
        compiler_params=limit,
        name="first",
    )(_stay(out_weight), own)
    middle = len(steps) // 2
    groups = [received[:middle], received[middle:-1] + handed[:middle], handed[middle:-1]]
    for group in groups:
        carry = pl.pallas_call(
            functools.partial(_more_kernel, len(group)),
            out_shape=state,
            in_specs=_vmem(3 + len(group)),
            out_specs=_vmem(2),
            scratch_shapes=[pltpu.VMEM((len(group) * lanes, columns), BF16)],
            compiler_params=limit,
        )(weight, *carry, *group)
    tile = (rows_here, residues, width)
    return pl.pallas_call(
        _last_kernel,
        out_shape=jax.ShapeDtypeStruct(tile, BF16),
        in_specs=_vmem(3) + [anywhere] * 2 + _vmem(2),
        out_specs=anywhere,
        scratch_shapes=[
            pltpu.VMEM((lanes, columns), BF16),
            pltpu.VMEM(crop.shape, crop.dtype),
            pltpu.VMEM((1, width), F32),
            pltpu.VMEM(tile, BF16),
            pltpu.SemaphoreType.DMA((2,)),
            pltpu.SemaphoreType.DMA((rows_here,)),
        ],
        compiler_params=limit,
        name="last",
    )(
        weight,
        *carry,
        _stay(crop),
        _stay(out_bias.reshape(1, -1)),
        received[-1],
        handed[-1],
    )


def solution(mesh):
    return jax.shard_map(
        per_device,
        mesh=mesh,
        in_specs=(
            P(("grp", "row"), None, None),
            P(("grp", "row")),
            P("grp"),
            P(),
            P(),
            P(),
            P(),
            P(),
            P(),
            P(),
            P(),
        ),
        out_specs=P(("grp", "row"), None, None),
        check_vma=False,
    )
```

```python
import functools

import jax
import jax.numpy as jnp
from jax import lax
from jax.experimental import pallas as pl
from jax.experimental.pallas import tpu as pltpu
from jax.sharding import PartitionSpec as P


F32 = jnp.float32
BF16 = jnp.bfloat16
FLAG_ROWS = 8


def _iota(shape, dim):
    return lax.broadcasted_iota(jnp.int32, shape, dim)


def _column(row):
    length = row.shape[1]
    square = (length, length)
    picked = jnp.where(
        _iota(square, 0) == _iota(square, 1), jnp.broadcast_to(row, square), 0.0
    )
    return jnp.sum(picked, axis=1, keepdims=True)


def _stay(array):
    return pltpu.with_memory_space_constraint(array, pltpu.HBM)


def _vmem(n):
    return [pl.BlockSpec(memory_space=pltpu.VMEM)] * n


def _project_kernel(
    x_hbm,
    flags_hbm,
    crop_hbm,
    gain_hbm,
    shift_hbm,
    wl_hbm,
    wr_hbm,
    lb_hbm,
    rb_hbm,
    out_ref,
    x_ref,
    flags_ref,
    crop_ref,
    gain_ref,
    shift_ref,
    wl_ref,
    wr_ref,
    lb_ref,
    rb_ref,
    x_sems,
    sems,
):
    seqs, residues, _ = x_ref.shape
    channels = wl_ref.shape[0]
    small = [
        pltpu.make_async_copy(src, dst, sems.at[n])
        for n, (src, dst) in enumerate(
            [
                (wr_hbm, wr_ref),
                (wl_hbm, wl_ref),
                (gain_hbm, gain_ref),
                (shift_hbm, shift_ref),
                (crop_hbm, crop_ref),
                (flags_hbm, flags_ref),
                (lb_hbm, lb_ref),
                (rb_hbm, rb_ref),
            ]
        )
    ]
    loads = [
        pltpu.make_async_copy(x_hbm.at[s], x_ref.at[s], x_sems.at[s]) for s in range(seqs)
    ]
    for copy in small + loads:
        copy.start()
    pair = 2 * seqs
    lanes = pair * channels
    first = (lax.axis_index("row") % 2) * seqs
    which = _iota((channels, lanes), 0)
    spread = _iota((channels, lanes), 1)
    pick_r = jnp.where(spread // pair == which, 1.0, 0.0)
    pick_l = jnp.where(spread % channels == which, 1.0, 0.0)
    exact = dict(precision=lax.Precision.HIGHEST, preferred_element_type=F32)
    lane = _iota((1, lanes), 1)
    seq_r = lane % pair - first
    seq_l = lane // channels - first
    for copy in small:
        copy.wait()
    turned = (((0,), (0,)), ((), ()))
    wr_rep = lax.dot_general(
        wr_ref[...], pick_r.astype(BF16), turned, preferred_element_type=F32
    ).astype(BF16)
    wl_rep = lax.dot_general(
        wl_ref[...], pick_l.astype(BF16), turned, preferred_element_type=F32
    ).astype(BF16)
    rb_rep = jnp.dot(jnp.broadcast_to(rb_ref[...], (8, channels)), pick_r, **exact)[0:1]
    lb_rep = jnp.dot(jnp.broadcast_to(lb_ref[...], (8, channels)), pick_l, **exact)[0:1]
    crop = _column(crop_ref[...].astype(F32))
    right = jnp.zeros((residues, lanes), F32)
    left = jnp.zeros((residues, lanes), F32)
    flag_r = jnp.zeros((1, lanes), F32)
    flag_l = jnp.zeros((1, lanes), F32)
    flag_row = jnp.zeros((1, lanes), F32)
    flags = flags_ref[...].astype(F32)
    for s in range(seqs):
        flag = jnp.broadcast_to(flags[:, s : s + 1], (1, lanes))
        flag_r = jnp.where(seq_r == s, flag, flag_r)
        flag_l = jnp.where(seq_l == s, flag, flag_l)
        flag_row = jnp.where(lane - first == s, flag, flag_row)
    for s in range(seqs):
        loads[s].wait()
        values = x_ref[s].astype(F32)
        values = values - jnp.mean(values, axis=-1, keepdims=True)
        variance = jnp.mean(values * values, axis=-1, keepdims=True)
        normed = values * lax.rsqrt(variance + 1e-05) * gain_ref[...] + shift_ref[...]
        high = normed.astype(BF16)
        low = (normed - high.astype(F32)).astype(BF16)
        to_right = jnp.dot(high, wr_rep, preferred_element_type=F32) + jnp.dot(
            low, wr_rep, preferred_element_type=F32
        )
        to_left = jnp.dot(high, wl_rep, preferred_element_type=F32) + jnp.dot(
            low, wl_rep, preferred_element_type=F32
        )
        right = jnp.where(seq_r == s, to_right, right)
        left = jnp.where(seq_l == s, to_left, left)
    out_ref[0:residues] = ((right + rb_rep) * (flag_r * crop)).astype(BF16)
    out_ref[residues : 2 * residues] = ((left + lb_rep) * (flag_l * crop)).astype(BF16)
    rows = _iota((2 * FLAG_ROWS, lanes), 0)
    out_ref[2 * residues :] = jnp.where(rows == 0, flag_row, 0.0).astype(BF16)


def _pack_kernel(steps, rows_chip, own_ref, other_ref, *out_refs):
    residues = own_ref.shape[0] // 2 - FLAG_ROWS
    total = rows_chip + FLAG_ROWS
    index = lax.axis_index("row")
    chip, core = index // 2, index % 2
    right = own_ref[0:residues] + other_ref[0:residues]
    flags = own_ref[2 * residues :] + other_ref[2 * residues :]
    for out_ref, (far, near) in zip(out_refs, ((0, 0),) + steps):
        target = chip ^ jnp.where(core == 1, far, near)
        start = pl.multiple_of(residues + target * rows_chip, rows_chip)
        out_ref[0:residues] = right
        slab = own_ref[pl.ds(start, rows_chip)] + other_ref[pl.ds(start, rows_chip)]
        tail = jnp.concatenate([slab.astype(F32), flags.astype(F32)], axis=0)
        out_ref[residues : residues + total] = tail[0:total].astype(BF16)


def _read(slot, rows):
    if not isinstance(slot, tuple):
        return slot[rows]
    north, south = slot
    return jnp.where(lax.axis_index("row") % 2 == 1, north[rows], south[rows])


def _rows(slot):
    return (slot[0] if isinstance(slot, tuple) else slot).shape


def _spread(slots, w_ref, a_ref):
    channels = w_ref.shape[0]
    height, lanes = _rows(slots[0])
    pair = lanes // channels
    width = w_ref.shape[1] // channels
    residues = height - 2 * pair - FLAG_ROWS
    core = lax.axis_index("row") % 2
    mine = _iota((pair, lanes), 1) // channels == _iota((pair, lanes), 0)
    rows = []
    for slot in slots:
        slab = _read(slot, slice(residues, residues + 2 * pair)).astype(F32)
        slab = jnp.where(core == 1, slab[pair:], slab[:pair])
        for i in range(pair):
            rows.append(jnp.where(mine, jnp.broadcast_to(slab[i : i + 1], (pair, lanes)), 0.0))
    spread = jnp.concatenate(rows, axis=0).astype(BF16)
    for e in range(0, channels, 2):
        block = w_ref[:, e * width : (e + 2) * width]
        product = jnp.dot(
            spread, jnp.concatenate([block] * pair, axis=0), preferred_element_type=F32
        )
        for n in range(len(slots)):
            for i in range(pair):
                at = (n * pair + i) * pair
                both = jnp.concatenate(
                    [product[at : at + pair, :width], product[at : at + pair, width:]], axis=0
                )
                a_ref[
                    n * lanes + e * pair : n * lanes + (e + 2) * pair,
                    i * width : (i + 1) * width,
                ] = both.astype(BF16)


def _contract(slots, a_ref, residues, columns=slice(None)):
    lanes = _rows(slots[0])[1]
    total = None
    for n, slot in enumerate(slots):
        part = jnp.dot(
            _read(slot, slice(0, residues)),
            a_ref[n * lanes : (n + 1) * lanes, columns],
            preferred_element_type=F32,
        )
        total = part if total is None else total + part
    return total


def _live(slots):
    total = None
    for slot in slots:
        rows = _rows(slot)[0]
        part = _read(slot, slice(rows - 2 * FLAG_ROWS, rows)).astype(F32)[FLAG_ROWS:]
        total = part if total is None else total + part
    return total


def _prepare_kernel(
    channels, raw_ref, crop_hbm, bias_hbm, w_ref, column_ref, own_ref, bias_ref, wide_ref, crop_ref, sems
):
    loads = [
        pltpu.make_async_copy(src, dst, sems.at[n])
        for n, (src, dst) in enumerate([(crop_hbm, crop_ref), (bias_hbm, bias_ref)])
    ]
    for copy in loads:
        copy.start()
    width = raw_ref.shape[1]
    wide_ref[...] = raw_ref[...].astype(F32)
    for e in range(channels):
        block = wide_ref[pl.ds(e, channels, stride=channels), :]
        w_ref[:, e * width : (e + 1) * width] = block.astype(BF16)
    for copy in loads:
        copy.wait()
    crop = crop_ref[...].astype(F32)
    column_ref[...] = jnp.broadcast_to(_column(crop), column_ref.shape)
    rows_here = own_ref.shape[0]
    square = (rows_here, crop.shape[1])
    mine = _iota(square, 1) - lax.axis_index("row") * rows_here == _iota(square, 0)
    kept = jnp.where(mine, jnp.broadcast_to(crop, square), 0.0)
    own_ref[...] = jnp.broadcast_to(jnp.sum(kept, axis=1, keepdims=True), own_ref.shape)


def _first_kernel(count, w_ref, *refs):
    slots, (sum_ref, live_ref, a_ref) = refs[:count], refs[count:]
    _spread(slots, w_ref, a_ref)
    sum_ref[...] = _contract(slots, a_ref, sum_ref.shape[0])
    live_ref[...] = _live(slots)


def _more_kernel(count, w_ref, sum_in, live_in, *refs):
    slots, (sum_ref, live_ref, a_ref) = refs[:count], refs[count:]
    _spread(slots, w_ref, a_ref)
    sum_ref[...] = sum_in[...] + _contract(slots, a_ref, sum_ref.shape[0])
    live_ref[...] = live_in[...] + _live(slots)


def _last_kernel(
    w_ref,
    column_ref,
    own_ref,
    bias_ref,
    sum_in,
    live_in,
    north_ref,
    south_ref,
    out_hbm,
    a_ref,
    out_ref,
    sems,
):
    slots = [(north_ref, south_ref)]
    rows_here, _, width = out_ref.shape
    flags = live_in[...] + _live(slots)
    live = jnp.sum(jnp.sum(flags, axis=1, keepdims=True), axis=0, keepdims=True)
    _spread(slots, w_ref, a_ref)
    stores = []
    group = 2 if rows_here % 2 == 0 else 1
    for first in range(0, rows_here, group):
        columns = slice(first * width, (first + group) * width)
        projected = sum_in[:, columns] + _contract(slots, a_ref, sum_in.shape[0], columns)
        for i in range(first, first + group):
            divisor = jnp.maximum(live * own_ref[i : i + 1] * column_ref[...], 1.0)
            part = projected[:, (i - first) * width : (i - first + 1) * width]
            out_ref[i] = (part / divisor + bias_ref[...]).astype(BF16)
            stores.append(pltpu.make_async_copy(out_ref.at[i], out_hbm.at[i], sems.at[i]))
            stores[-1].start()
    for copy in stores:
        copy.wait()


def per_device(
    alignment,
    seq_flags,
    crop_flags,
    norm_gain,
    norm_bias,
    left_weight,
    left_bias,
    right_weight,
    right_bias,
    out_weight,
    out_bias,
):
    seqs, residues, _ = alignment.shape
    channels = left_weight.shape[1]
    width = out_weight.shape[1]
    devices = lax.axis_size("row")
    rows_here = residues // devices
    rows_chip = 2 * rows_here
    chips = devices // 2
    lanes = 2 * seqs * channels
    half, quarter = chips // 2, max(1, chips // 4)
    steps = tuple(
        zip(
            [quarter] + [k for k in range(chips - 1, half, -1) if k != quarter],
            [k for k in range(half, 0, -1) if k != quarter] + [0],
        )
    )
    cores = [(d, d ^ 1) for d in range(devices)]
    crop = crop_flags.reshape(1, residues)
    limit = pltpu.CompilerParams(vmem_limit_bytes=48 * 1024 * 1024)
    anywhere = pl.BlockSpec(memory_space=pltpu.HBM)

    operands = (
        alignment,
        seq_flags.reshape(1, seqs),
        crop,
        norm_gain.reshape(1, -1),
        norm_bias.reshape(1, -1),
        left_weight.T,
        right_weight.T,
        left_bias.reshape(1, -1),
        right_bias.reshape(1, -1),
    )
    projected = pl.pallas_call(
        _project_kernel,
        out_shape=jax.ShapeDtypeStruct((2 * residues + 2 * FLAG_ROWS, lanes), BF16),
        in_specs=[anywhere] * len(operands),
        out_specs=_vmem(1)[0],
        scratch_shapes=[pltpu.VMEM(a.shape, a.dtype) for a in operands]
        + [pltpu.SemaphoreType.DMA((seqs,)), pltpu.SemaphoreType.DMA((len(operands) - 1,))],
        compiler_params=limit,
        name="project",
    )(*map(_stay, operands))
    other = lax.ppermute(projected, "row", cores)
    parcel = jax.ShapeDtypeStruct((residues + rows_chip + FLAG_ROWS, lanes), BF16)
    own, *parcels = pl.pallas_call(
        functools.partial(_pack_kernel, steps, rows_chip),
        out_shape=[parcel] * (1 + len(steps)),
        in_specs=_vmem(2),
        out_specs=_vmem(1 + len(steps)),
        compiler_params=limit,
        name="pack",
    )(projected, other)
    received, handed = [], []
    for (far, near), piece in zip(steps, parcels):
        pairs = [(2 * q + 1, 2 * (q ^ far) + 1) for q in range(chips)]
        back = [(2 * q + 1, 2 * q) for q in range(chips)]
        if near:
            pairs += [(2 * q, 2 * (q ^ near)) for q in range(chips)]
            back += [(2 * q, 2 * q + 1) for q in range(chips)]
        received.append(lax.ppermute(piece, "row", pairs))
        handed.append(lax.ppermute(received[-1], "row", back))

    columns = rows_here * width
    state = [
        jax.ShapeDtypeStruct((residues, columns), F32),
        jax.ShapeDtypeStruct((FLAG_ROWS, lanes), F32),
    ]
    weight, *spread = pl.pallas_call(
        functools.partial(_prepare_kernel, channels),
        out_shape=[
            jax.ShapeDtypeStruct((channels, channels * width), BF16),
            jax.ShapeDtypeStruct((residues, width), F32),
            jax.ShapeDtypeStruct((rows_here, width), F32),
            jax.ShapeDtypeStruct((1, width), F32),
        ],
        in_specs=_vmem(1) + [anywhere] * 2,
        out_specs=_vmem(4),
        scratch_shapes=[
            pltpu.VMEM(out_weight.shape, F32),
            pltpu.VMEM(crop.shape, crop.dtype),
            pltpu.SemaphoreType.DMA((2,)),
        ],
        compiler_params=limit,
        name="prepare",
    )(out_weight, _stay(crop), _stay(out_bias.reshape(1, -1)))

    middle = len(steps) // 2
    early = [own] + received[:-1] + handed[:middle]
    carry = pl.pallas_call(
        functools.partial(_first_kernel, len(early)),
        out_shape=state,
        in_specs=_vmem(1 + len(early)),
        out_specs=_vmem(2),
        scratch_shapes=[pltpu.VMEM((len(early) * lanes, columns), BF16)],
        compiler_params=limit,
        name="early",
    )(weight, *early)
    late = handed[middle:-1]
    carry = pl.pallas_call(
        functools.partial(_more_kernel, len(late)),
        out_shape=state,
        in_specs=_vmem(3 + len(late)),
        out_specs=_vmem(2),
        scratch_shapes=[pltpu.VMEM((len(late) * lanes, columns), BF16)],
        compiler_params=limit,
        name="late",
    )(weight, *carry, *late)
    tile = (rows_here, residues, width)
    return pl.pallas_call(
        _last_kernel,
        out_shape=jax.ShapeDtypeStruct(tile, BF16),
        in_specs=_vmem(8),
        out_specs=anywhere,
        scratch_shapes=[
            pltpu.VMEM((lanes, columns), BF16),
            pltpu.VMEM(tile, BF16),
            pltpu.SemaphoreType.DMA((rows_here,)),
        ],
        compiler_params=limit,
        name="last",
    )(weight, *spread, *carry, received[-1], handed[-1])


def solution(mesh):
    return jax.shard_map(
        per_device,
        mesh=mesh,
        in_specs=(
            P(("grp", "row"), None, None),
            P(("grp", "row")),
            P("grp"),
            P(),
            P(),
            P(),
            P(),
            P(),
            P(),
            P(),
            P(),
        ),
        out_specs=P(("grp", "row"), None, None),
        check_vma=False,
    )
```

```python
import functools

import jax
import jax.numpy as jnp
from jax import lax
from jax.experimental import pallas as pl
from jax.experimental.pallas import tpu as pltpu
from jax.sharding import PartitionSpec as P


F32 = jnp.float32
BF16 = jnp.bfloat16
FLAG_ROWS = 8


def _iota(shape, dim):
    return lax.broadcasted_iota(jnp.int32, shape, dim)


def _column(row):
    length = row.shape[1]
    square = (length, length)
    picked = jnp.where(
        _iota(square, 0) == _iota(square, 1), jnp.broadcast_to(row, square), 0.0
    )
    return jnp.sum(picked, axis=1, keepdims=True)


def _stay(array):
    return pltpu.with_memory_space_constraint(array, pltpu.HBM)


def _vmem(n):
    return [pl.BlockSpec(memory_space=pltpu.VMEM)] * n


def _project_kernel(
    x_hbm,
    flags_hbm,
    crop_hbm,
    gain_hbm,
    shift_hbm,
    wl_hbm,
    wr_hbm,
    lb_hbm,
    rb_hbm,
    out_ref,
    x_ref,
    flags_ref,
    crop_ref,
    gain_ref,
    shift_ref,
    wl_ref,
    wr_ref,
    lb_ref,
    rb_ref,
    x_sems,
    sems,
):
    seqs, residues, _ = x_ref.shape
    channels = wl_ref.shape[0]
    small = [
        pltpu.make_async_copy(src, dst, sems.at[n])
        for n, (src, dst) in enumerate(
            [
                (wr_hbm, wr_ref),
                (wl_hbm, wl_ref),
                (gain_hbm, gain_ref),
                (shift_hbm, shift_ref),
                (crop_hbm, crop_ref),
                (flags_hbm, flags_ref),
                (lb_hbm, lb_ref),
                (rb_hbm, rb_ref),
            ]
        )
    ]
    loads = [
        pltpu.make_async_copy(x_hbm.at[s], x_ref.at[s], x_sems.at[s]) for s in range(seqs)
    ]
    for copy in small + loads:
        copy.start()
    pair = 2 * seqs
    lanes = pair * channels
    first = (lax.axis_index("row") % 2) * seqs
    which = _iota((channels, lanes), 0)
    spread = _iota((channels, lanes), 1)
    pick_r = jnp.where(spread // pair == which, 1.0, 0.0)
    pick_l = jnp.where(spread % channels == which, 1.0, 0.0)
    exact = dict(precision=lax.Precision.HIGHEST, preferred_element_type=F32)
    lane = _iota((1, lanes), 1)
    seq_r = lane % pair - first
    seq_l = lane // channels - first
    for copy in small:
        copy.wait()
    turned = (((0,), (0,)), ((), ()))
    weights = jnp.concatenate(
        [
            lax.dot_general(ref[...], pick.astype(BF16), turned, preferred_element_type=F32)
            for ref, pick in ((wr_ref, pick_r), (wl_ref, pick_l))
        ],
        axis=1,
    ).astype(BF16)
    weights = jnp.concatenate([weights, weights], axis=0)
    rb_rep = jnp.dot(jnp.broadcast_to(rb_ref[...], (8, channels)), pick_r, **exact)[0:1]
    lb_rep = jnp.dot(jnp.broadcast_to(lb_ref[...], (8, channels)), pick_l, **exact)[0:1]
    crop = _column(crop_ref[...].astype(F32))
    right = jnp.zeros((residues, lanes), F32)
    left = jnp.zeros((residues, lanes), F32)
    flag_r = jnp.zeros((1, lanes), F32)
    flag_l = jnp.zeros((1, lanes), F32)
    flag_row = jnp.zeros((1, lanes), F32)
    flags = flags_ref[...].astype(F32)
    for s in range(seqs):
        flag = jnp.broadcast_to(flags[:, s : s + 1], (1, lanes))
        flag_r = jnp.where(seq_r == s, flag, flag_r)
        flag_l = jnp.where(seq_l == s, flag, flag_l)
        flag_row = jnp.where(lane - first == s, flag, flag_row)
    for copy in loads:
        copy.wait()
    rows = []
    for s in range(seqs):
        values = x_ref[s].astype(F32)
        values = values - jnp.mean(values, axis=-1, keepdims=True)
        variance = jnp.mean(values * values, axis=-1, keepdims=True)
        normed = values * lax.rsqrt(variance + 1e-05) * gain_ref[...] + shift_ref[...]
        high = normed.astype(BF16)
        low = (normed - high.astype(F32)).astype(BF16)
        rows.append(jnp.concatenate([high, low], axis=1))
    product = jnp.dot(jnp.concatenate(rows, axis=0), weights, preferred_element_type=F32)
    for s in range(seqs):
        part = product[s * residues : (s + 1) * residues]
        right = jnp.where(seq_r == s, part[:, :lanes], right)
        left = jnp.where(seq_l == s, part[:, lanes:], left)
    out_ref[0:residues] = ((right + rb_rep) * (flag_r * crop)).astype(BF16)
    out_ref[residues : 2 * residues] = ((left + lb_rep) * (flag_l * crop)).astype(BF16)
    rows = _iota((2 * FLAG_ROWS, lanes), 0)
    out_ref[2 * residues :] = jnp.where(rows == 0, flag_row, 0.0).astype(BF16)


def _pack_kernel(steps, rows_chip, own_ref, other_ref, *out_refs):
    residues = own_ref.shape[0] // 2 - FLAG_ROWS
    half, rows_here = residues // 2, rows_chip // 2
    index = lax.axis_index("row")
    chip, core = index // 2, index % 2
    right = own_ref[0:residues] + other_ref[0:residues]
    flags = (own_ref[2 * residues :] + other_ref[2 * residues :]).astype(F32)[:FLAG_ROWS]
    for out_ref, (far, near) in zip(out_refs, ((0, 0),) + steps):
        target = chip ^ jnp.where(core == 1, far, near)
        start = pl.multiple_of(residues + target * rows_chip, rows_chip)
        slab = own_ref[pl.ds(start, rows_chip)] + other_ref[pl.ds(start, rows_chip)]
        slab = slab.astype(F32)
        if out_ref.shape[0] > residues:
            out_ref[0:residues] = right
            out_ref[residues:] = jnp.concatenate([slab, flags], axis=0).astype(BF16)
        else:
            out_ref[0:half] = jnp.where(core == 1, right[:half], right[half:])
            slab = jnp.where(core == 1, slab[rows_here:], slab[:rows_here])
            out_ref[half:] = jnp.concatenate([slab, flags], axis=0).astype(BF16)


def _spread(slabs, w_ref, targets):
    channels = w_ref.shape[0]
    rows_here, lanes = slabs[0].shape
    pair = lanes // channels
    width = w_ref.shape[1] // channels
    mine = _iota((pair, lanes), 1) // channels == _iota((pair, lanes), 0)
    rows = []
    for slab in slabs:
        for i in range(rows_here):
            rows.append(jnp.where(mine, jnp.broadcast_to(slab[i : i + 1], (pair, lanes)), 0.0))
    spread = jnp.concatenate(rows, axis=0).astype(BF16)
    for e in range(0, channels, 2):
        block = w_ref[:, e * width : (e + 2) * width]
        product = jnp.dot(
            spread, jnp.concatenate([block] * pair, axis=0), preferred_element_type=F32
        )
        for n, (a_ref, base) in enumerate(targets):
            for i in range(rows_here):
                at = (n * rows_here + i) * pair
                both = jnp.concatenate(
                    [product[at : at + pair, :width], product[at : at + pair, width:]], axis=0
                )
                a_ref[
                    base + e * pair : base + (e + 2) * pair, i * width : (i + 1) * width
                ] = both.astype(BF16)


def _slab(ref, residues):
    both = ref[residues : ref.shape[0] - FLAG_ROWS].astype(F32)
    half = both.shape[0] // 2
    return jnp.where(lax.axis_index("row") % 2 == 1, both[half:], both[:half])


def _contract(refs, a_ref, residues):
    lanes = refs[0].shape[1]
    total = None
    for n, ref in enumerate(refs):
        part = jnp.dot(
            ref[0:residues], a_ref[n * lanes : (n + 1) * lanes], preferred_element_type=F32
        )
        total = part if total is None else total + part
    return total


def _flags(refs):
    total = None
    for ref in refs:
        part = ref[ref.shape[0] - 2 * FLAG_ROWS :].astype(F32)[FLAG_ROWS:]
        total = part if total is None else total + part
    return total


def _prepare_kernel(
    channels, raw_ref, crop_hbm, bias_hbm, w_ref, column_ref, own_ref, bias_ref, wide_ref, crop_ref, sems
):
    loads = [
        pltpu.make_async_copy(src, dst, sems.at[n])
        for n, (src, dst) in enumerate([(crop_hbm, crop_ref), (bias_hbm, bias_ref)])
    ]
    for copy in loads:
        copy.start()
    width = raw_ref.shape[1]
    wide_ref[...] = raw_ref[...].astype(F32)
    for e in range(channels):
        block = wide_ref[pl.ds(e, channels, stride=channels), :]
        w_ref[:, e * width : (e + 1) * width] = block.astype(BF16)
    for copy in loads:
        copy.wait()
    crop = crop_ref[...].astype(F32)
    column_ref[...] = jnp.broadcast_to(_column(crop), column_ref.shape)
    rows_here = own_ref.shape[0]
    square = (rows_here, crop.shape[1])
    mine = _iota(square, 1) - lax.axis_index("row") * rows_here == _iota(square, 0)
    kept = jnp.where(mine, jnp.broadcast_to(crop, square), 0.0)
    own_ref[...] = jnp.broadcast_to(jnp.sum(kept, axis=1, keepdims=True), own_ref.shape)


def _early_kernel(count, w_ref, *refs):
    parcels, (sum_ref, flags_ref, a_ref) = refs[:count], refs[count:]
    residues, lanes = sum_ref.shape[0], parcels[0].shape[1]
    slabs = [_slab(ref, residues) for ref in parcels]
    _spread(slabs, w_ref, [(a_ref, n * lanes) for n in range(count)])
    sum_ref[...] = _contract(parcels, a_ref, residues)
    flags_ref[...] = _flags(parcels)


def _late_kernel(count, w_ref, sum_in, flags_in, shared_ref, *refs):
    parcels, (sum_ref, flags_ref, shared_a_ref, a_ref) = refs[:count], refs[count:]
    residues, lanes = sum_ref.shape[0], parcels[0].shape[1]
    slabs = [_slab(ref, residues) for ref in parcels]
    slabs.append(shared_ref[residues // 2 :].astype(F32)[:-FLAG_ROWS])
    targets = [(a_ref, n * lanes) for n in range(count)] + [(shared_a_ref, 0)]
    _spread(slabs, w_ref, targets)
    sum_ref[...] = sum_in[...] + _contract(parcels, a_ref, residues)
    flags_ref[...] = flags_in[...] + _flags(parcels + (shared_ref,))


def _last_kernel(
    column_ref,
    own_ref,
    bias_ref,
    sum_in,
    flags_in,
    a_ref,
    mine_ref,
    other_ref,
    out_hbm,
    out_ref,
    sems,
):
    rows_here, residues, width = out_ref.shape
    half = residues // 2
    core = lax.axis_index("row") % 2
    mine, other = mine_ref[0:half], other_ref[0:half]
    right = jnp.concatenate(
        [jnp.where(core == 1, mine, other), jnp.where(core == 1, other, mine)], axis=0
    )
    live = jnp.sum(jnp.sum(flags_in[...], axis=1, keepdims=True), axis=0, keepdims=True)
    stores = []
    group = 2 if rows_here % 2 == 0 else 1
    for first in range(0, rows_here, group):
        columns = slice(first * width, (first + group) * width)
        projected = sum_in[:, columns] + jnp.dot(
            right, a_ref[:, columns], preferred_element_type=F32
        )
        for i in range(first, first + group):
            divisor = jnp.maximum(live * own_ref[i : i + 1] * column_ref[...], 1.0)
            part = projected[:, (i - first) * width : (i - first + 1) * width]
            out_ref[i] = (part / divisor + bias_ref[...]).astype(BF16)
            stores.append(pltpu.make_async_copy(out_ref.at[i], out_hbm.at[i], sems.at[i]))
            stores[-1].start()
    for copy in stores:
        copy.wait()


def per_device(
    alignment,
    seq_flags,
    crop_flags,
    norm_gain,
    norm_bias,
    left_weight,
    left_bias,
    right_weight,
    right_bias,
    out_weight,
    out_bias,
):
    seqs, residues, _ = alignment.shape
    channels = left_weight.shape[1]
    width = out_weight.shape[1]
    devices = lax.axis_size("row")
    rows_here = residues // devices
    rows_chip = 2 * rows_here
    chips = devices // 2
    lanes = 2 * seqs * channels
    half, quarter = chips // 2, max(1, chips // 4)
    steps = tuple(
        zip(
            [quarter] + [k for k in range(chips - 1, half, -1) if k != quarter],
            [k for k in range(half, 0, -1) if k != quarter] + [half + 1],
        )
    )
    cores = [(d, d ^ 1) for d in range(devices)]
    crop = crop_flags.reshape(1, residues)
    limit = pltpu.CompilerParams(vmem_limit_bytes=48 * 1024 * 1024)
    anywhere = pl.BlockSpec(memory_space=pltpu.HBM)

    operands = (
        alignment,
        seq_flags.reshape(1, seqs),
        crop,
        norm_gain.reshape(1, -1),
        norm_bias.reshape(1, -1),
        left_weight.T,
        right_weight.T,
        left_bias.reshape(1, -1),
        right_bias.reshape(1, -1),
    )
    projected = pl.pallas_call(
        _project_kernel,
        out_shape=jax.ShapeDtypeStruct((2 * residues + 2 * FLAG_ROWS, lanes), BF16),
        in_specs=[anywhere] * len(operands),
        out_specs=_vmem(1)[0],
        scratch_shapes=[pltpu.VMEM(a.shape, a.dtype) for a in operands]
        + [pltpu.SemaphoreType.DMA((seqs,)), pltpu.SemaphoreType.DMA((len(operands) - 1,))],
        compiler_params=limit,
        name="project",
    )(*map(_stay, operands))
    other = lax.ppermute(projected, "row", cores)
    parcel = jax.ShapeDtypeStruct((residues + rows_chip + FLAG_ROWS, lanes), BF16)
    shared = jax.ShapeDtypeStruct((residues // 2 + rows_here + FLAG_ROWS, lanes), BF16)
    own, *parcels = pl.pallas_call(
        functools.partial(_pack_kernel, steps, rows_chip),
        out_shape=[parcel] * len(steps) + [shared],
        in_specs=_vmem(2),
        out_specs=_vmem(1 + len(steps)),
        compiler_params=limit,
        name="pack",
    )(projected, other)
    received, handed = [], []
    for (far, near), piece in zip(steps, parcels):
        pairs = [(2 * q + 1, 2 * (q ^ far) + 1) for q in range(chips)]
        pairs += [(2 * q, 2 * (q ^ near)) for q in range(chips)]
        received.append(lax.ppermute(piece, "row", pairs))
        handed.append(lax.ppermute(received[-1], "row", cores))

    columns = rows_here * width
    state = [
        jax.ShapeDtypeStruct((residues, columns), F32),
        jax.ShapeDtypeStruct((FLAG_ROWS, lanes), F32),
    ]
    weight, *spread = pl.pallas_call(
        functools.partial(_prepare_kernel, channels),
        out_shape=[
            jax.ShapeDtypeStruct((channels, channels * width), BF16),
            jax.ShapeDtypeStruct((residues, width), F32),
            jax.ShapeDtypeStruct((rows_here, width), F32),
            jax.ShapeDtypeStruct((1, width), F32),
        ],
        in_specs=_vmem(1) + [anywhere] * 2,
        out_specs=_vmem(4),
        scratch_shapes=[
            pltpu.VMEM(out_weight.shape, F32),
            pltpu.VMEM(crop.shape, crop.dtype),
            pltpu.SemaphoreType.DMA((2,)),
        ],
        compiler_params=limit,
        name="prepare",
    )(out_weight, _stay(crop), _stay(out_bias.reshape(1, -1)))

    early = [own] + received[:-1]
    carry = pl.pallas_call(
        functools.partial(_early_kernel, len(early)),
        out_shape=state,
        in_specs=_vmem(1 + len(early)),
        out_specs=_vmem(2),
        scratch_shapes=[pltpu.VMEM((len(early) * lanes, columns), BF16)],
        compiler_params=limit,
        name="early",
    )(weight, *early)
    late = handed[:-1]
    carry = pl.pallas_call(
        functools.partial(_late_kernel, len(late)),
        out_shape=state + [jax.ShapeDtypeStruct((lanes, columns), BF16)],
        in_specs=_vmem(4 + len(late)),
        out_specs=_vmem(3),
        scratch_shapes=[pltpu.VMEM((len(late) * lanes, columns), BF16)],
        compiler_params=limit,
        name="late",
    )(weight, *carry, received[-1], *late)
    tile = (rows_here, residues, width)
    return pl.pallas_call(
        _last_kernel,
        out_shape=jax.ShapeDtypeStruct(tile, BF16),
        in_specs=_vmem(8),
        out_specs=anywhere,
        scratch_shapes=[
            pltpu.VMEM(tile, BF16),
            pltpu.SemaphoreType.DMA((rows_here,)),
        ],
        compiler_params=limit,
        name="last",
    )(*spread, *carry, received[-1], handed[-1])


def solution(mesh):
    return jax.shard_map(
        per_device,
        mesh=mesh,
        in_specs=(
            P(("grp", "row"), None, None),
            P(("grp", "row")),
            P("grp"),
            P(),
            P(),
            P(),
            P(),
            P(),
            P(),
            P(),
            P(),
        ),
        out_specs=P(("grp", "row"), None, None),
        check_vma=False,
    )
```

```python
import functools

import jax
import jax.numpy as jnp
from jax import lax
from jax.experimental import pallas as pl
from jax.experimental.pallas import tpu as pltpu
from jax.sharding import PartitionSpec as P


F32 = jnp.float32
BF16 = jnp.bfloat16
FLAG_ROWS = 8


def _iota(shape, dim):
    return lax.broadcasted_iota(jnp.int32, shape, dim)


def _column(row):
    length = row.shape[1]
    square = (length, length)
    picked = jnp.where(
        _iota(square, 0) == _iota(square, 1), jnp.broadcast_to(row, square), 0.0
    )
    return jnp.sum(picked, axis=1, keepdims=True)


def _pick_lanes(row, pick):
    high = row.astype(BF16).astype(F32)
    middle = (row - high).astype(BF16).astype(F32)
    parts = jnp.concatenate([high, middle, row - high - middle, jnp.zeros_like(row)], axis=0)
    parts = jnp.concatenate([parts, jnp.zeros_like(parts)], axis=0).astype(BF16)
    return jnp.sum(jnp.dot(parts, pick, preferred_element_type=F32), axis=0, keepdims=True)


def _stay(array):
    return pltpu.with_memory_space_constraint(array, pltpu.HBM)


def _vmem(n):
    return [pl.BlockSpec(memory_space=pltpu.VMEM)] * n


def _project_kernel(
    x_hbm,
    flags_hbm,
    crop_hbm,
    gain_hbm,
    shift_hbm,
    wl_hbm,
    wr_hbm,
    lb_hbm,
    rb_hbm,
    out_ref,
    x_ref,
    flags_ref,
    crop_ref,
    gain_ref,
    shift_ref,
    wl_ref,
    wr_ref,
    lb_ref,
    rb_ref,
    x_sems,
    sems,
):
    seqs, residues, _ = x_ref.shape
    channels = wl_ref.shape[0]
    small = [
        pltpu.make_async_copy(src, dst, sems.at[n])
        for n, (src, dst) in enumerate(
            [
                (wr_hbm, wr_ref),
                (wl_hbm, wl_ref),
                (gain_hbm, gain_ref),
                (shift_hbm, shift_ref),
                (crop_hbm, crop_ref),
                (flags_hbm, flags_ref),
                (lb_hbm, lb_ref),
                (rb_hbm, rb_ref),
            ]
        )
    ]
    loads = [
        pltpu.make_async_copy(x_hbm, x_ref, x_sems.at[0])
    ]
    for copy in small + loads:
        copy.start()
    pair = 2 * seqs
    lanes = pair * channels
    first = (lax.axis_index("row") % 2) * seqs
    which = _iota((channels, lanes), 0)
    spread = _iota((channels, lanes), 1)
    pick_r = jnp.where(spread // pair == which, 1.0, 0.0).astype(BF16)
    pick_l = jnp.where(spread % channels == which, 1.0, 0.0).astype(BF16)
    lane = _iota((1, lanes), 1)
    seq_r = lane % pair - first
    seq_l = lane // channels - first
    for copy in small:
        copy.wait()
    turned = (((0,), (0,)), ((), ()))
    weights = jnp.concatenate(
        [
            lax.dot_general(ref[...], pick, turned, preferred_element_type=F32)
            for ref, pick in ((wr_ref, pick_r), (wl_ref, pick_l))
        ],
        axis=1,
    ).astype(BF16)
    weights = jnp.concatenate([weights, weights], axis=0)
    rb_rep = _pick_lanes(rb_ref[...], pick_r)
    lb_rep = _pick_lanes(lb_ref[...], pick_l)
    crop = _column(crop_ref[...].astype(F32))
    right = jnp.zeros((residues, lanes), F32)
    left = jnp.zeros((residues, lanes), F32)
    flag_r = jnp.zeros((1, lanes), F32)
    flag_l = jnp.zeros((1, lanes), F32)
    flag_row = jnp.zeros((1, lanes), F32)
    flags = flags_ref[...].astype(F32)
    for s in range(seqs):
        flag = jnp.broadcast_to(flags[:, s : s + 1], (1, lanes))
        flag_r = jnp.where(seq_r == s, flag, flag_r)
        flag_l = jnp.where(seq_l == s, flag, flag_l)
        flag_row = jnp.where(lane - first == s, flag, flag_row)
    for copy in loads:
        copy.wait()
    rows = []
    for s in range(seqs):
        values = x_ref[s].astype(F32)
        values = values - jnp.mean(values, axis=-1, keepdims=True)
        variance = jnp.mean(values * values, axis=-1, keepdims=True)
        normed = values * lax.rsqrt(variance + 1e-05) * gain_ref[...] + shift_ref[...]
        high = normed.astype(BF16)
        low = (normed - high.astype(F32)).astype(BF16)
        rows.append(jnp.concatenate([high, low], axis=1))
    product = jnp.dot(jnp.concatenate(rows, axis=0), weights, preferred_element_type=F32)
    for s in range(seqs):
        part = product[s * residues : (s + 1) * residues]
        right = jnp.where(seq_r == s, part[:, :lanes], right)
        left = jnp.where(seq_l == s, part[:, lanes:], left)
    out_ref[0:residues] = ((right + rb_rep) * (flag_r * crop)).astype(BF16)
    out_ref[residues : 2 * residues] = ((left + lb_rep) * (flag_l * crop)).astype(BF16)
    rows = _iota((2 * FLAG_ROWS, lanes), 0)
    out_ref[2 * residues :] = jnp.where(rows == 0, flag_row, 0.0).astype(BF16)


def _pack_kernel(steps, rows_chip, own_ref, other_ref, *out_refs):
    residues = own_ref.shape[0] // 2 - FLAG_ROWS
    half, rows_here = residues // 2, rows_chip // 2
    index = lax.axis_index("row")
    chip, core = index // 2, index % 2
    right = own_ref[0:residues] + other_ref[0:residues]
    flags = (own_ref[2 * residues :] + other_ref[2 * residues :]).astype(F32)[:FLAG_ROWS]
    for out_ref, (far, near) in zip(out_refs, ((0, 0),) + steps):
        target = chip ^ jnp.where(core == 1, far, near)
        start = pl.multiple_of(residues + target * rows_chip, rows_chip)
        slab = own_ref[pl.ds(start, rows_chip)] + other_ref[pl.ds(start, rows_chip)]
        slab = slab.astype(F32)
        if out_ref.shape[0] > residues:
            out_ref[0:residues] = right
            out_ref[residues:] = jnp.concatenate([slab, flags], axis=0).astype(BF16)
        else:
            out_ref[0:half] = jnp.where(core == 1, right[:half], right[half:])
            slab = jnp.where(core == 1, slab[rows_here:], slab[:rows_here])
            out_ref[half:] = jnp.concatenate([slab, flags], axis=0).astype(BF16)


def _spread(slabs, w_ref, targets):
    channels = w_ref.shape[0]
    rows_here, lanes = slabs[0].shape
    pair = lanes // channels
    width = w_ref.shape[1] // channels
    mine = _iota((pair, lanes), 1) // channels == _iota((pair, lanes), 0)
    rows = []
    for slab in slabs:
        for i in range(rows_here):
            rows.append(jnp.where(mine, jnp.broadcast_to(slab[i : i + 1], (pair, lanes)), 0.0))
    spread = jnp.concatenate(rows, axis=0).astype(BF16)
    for e in range(0, channels, 2):
        block = w_ref[:, e * width : (e + 2) * width]
        product = jnp.dot(
            spread, jnp.concatenate([block] * pair, axis=0), preferred_element_type=F32
        )
        for n, (a_ref, base) in enumerate(targets):
            for i in range(rows_here):
                at = (n * rows_here + i) * pair
                both = jnp.concatenate(
                    [product[at : at + pair, :width], product[at : at + pair, width:]], axis=0
                )
                a_ref[
                    base + e * pair : base + (e + 2) * pair, i * width : (i + 1) * width
                ] = both.astype(BF16)


def _slab(ref, residues):
    both = ref[residues : ref.shape[0] - FLAG_ROWS].astype(F32)
    half = both.shape[0] // 2
    return jnp.where(lax.axis_index("row") % 2 == 1, both[half:], both[:half])


def _contract(refs, a_ref, residues):
    lanes = refs[0].shape[1]
    total = None
    for n, ref in enumerate(refs):
        part = jnp.dot(
            ref[0:residues], a_ref[n * lanes : (n + 1) * lanes], preferred_element_type=F32
        )
        total = part if total is None else total + part
    return total


def _flags(refs):
    total = None
    for ref in refs:
        part = ref[ref.shape[0] - 2 * FLAG_ROWS :].astype(F32)[FLAG_ROWS:]
        total = part if total is None else total + part
    return total


def _prepare_kernel(
    channels, raw_ref, crop_hbm, bias_hbm, w_ref, column_ref, own_ref, bias_ref, wide_ref, crop_ref, sems
):
    loads = [
        pltpu.make_async_copy(src, dst, sems.at[n])
        for n, (src, dst) in enumerate([(crop_hbm, crop_ref), (bias_hbm, bias_ref)])
    ]
    for copy in loads:
        copy.start()
    width = raw_ref.shape[1]
    wide_ref[...] = raw_ref[...].astype(F32)
    for e in range(channels):
        block = wide_ref[pl.ds(e, channels, stride=channels), :]
        w_ref[:, e * width : (e + 1) * width] = block.astype(BF16)
    for copy in loads:
        copy.wait()
    crop = crop_ref[...].astype(F32)
    column_ref[...] = jnp.broadcast_to(_column(crop), column_ref.shape)
    rows_here = own_ref.shape[0]
    square = (rows_here, crop.shape[1])
    mine = _iota(square, 1) - lax.axis_index("row") * rows_here == _iota(square, 0)
    kept = jnp.where(mine, jnp.broadcast_to(crop, square), 0.0)
    own_ref[...] = jnp.broadcast_to(jnp.sum(kept, axis=1, keepdims=True), own_ref.shape)


def _early_kernel(count, w_ref, *refs):
    parcels, (sum_ref, flags_ref, a_ref) = refs[:count], refs[count:]
    residues, lanes = sum_ref.shape[0], parcels[0].shape[1]
    slabs = [_slab(ref, residues) for ref in parcels]
    _spread(slabs, w_ref, [(a_ref, n * lanes) for n in range(count)])
    sum_ref[...] = _contract(parcels, a_ref, residues)
    flags_ref[...] = _flags(parcels)


def _late_kernel(count, w_ref, sum_in, flags_in, shared_ref, *refs):
    parcels, (sum_ref, flags_ref, shared_a_ref, a_ref) = refs[:count], refs[count:]
    residues, lanes = sum_ref.shape[0], parcels[0].shape[1]
    slabs = [_slab(ref, residues) for ref in parcels]
    slabs.append(shared_ref[residues // 2 :].astype(F32)[:-FLAG_ROWS])
    targets = [(a_ref, n * lanes) for n in range(count)] + [(shared_a_ref, 0)]
    _spread(slabs, w_ref, targets)
    sum_ref[...] = sum_in[...] + _contract(parcels, a_ref, residues)
    flags_ref[...] = flags_in[...] + _flags(parcels + (shared_ref,))


def _last_kernel(
    column_ref,
    own_ref,
    bias_ref,
    sum_in,
    flags_in,
    a_ref,
    mine_ref,
    other_ref,
    out_hbm,
    out_ref,
    sems,
):
    rows_here, residues, width = out_ref.shape
    half = residues // 2
    core = lax.axis_index("row") % 2
    mine, other = mine_ref[0:half], other_ref[0:half]
    right = jnp.concatenate(
        [jnp.where(core == 1, mine, other), jnp.where(core == 1, other, mine)], axis=0
    )
    live = jnp.sum(jnp.sum(flags_in[...], axis=1, keepdims=True), axis=0, keepdims=True)
    inside = jnp.where(column_ref[...] > 0.0, 1.0 / jnp.maximum(live, 1.0), 1.0)
    stores = []
    group = 2 if rows_here % 2 == 0 else 1
    for first in range(0, rows_here, group):
        columns = slice(first * width, (first + group) * width)
        projected = sum_in[:, columns] + jnp.dot(
            right, a_ref[:, columns], preferred_element_type=F32
        )
        for i in range(first, first + group):
            scale = jnp.where(own_ref[i : i + 1] > 0.0, inside, 1.0)
            part = projected[:, (i - first) * width : (i - first + 1) * width]
            out_ref[i] = (part * scale + bias_ref[...]).astype(BF16)
            stores.append(pltpu.make_async_copy(out_ref.at[i], out_hbm.at[i], sems.at[i]))
            stores[-1].start()
    for copy in stores:
        copy.wait()


def per_device(
    alignment,
    seq_flags,
    crop_flags,
    norm_gain,
    norm_bias,
    left_weight,
    left_bias,
    right_weight,
    right_bias,
    out_weight,
    out_bias,
):
    seqs, residues, _ = alignment.shape
    channels = left_weight.shape[1]
    width = out_weight.shape[1]
    devices = lax.axis_size("row")
    rows_here = residues // devices
    rows_chip = 2 * rows_here
    chips = devices // 2
    lanes = 2 * seqs * channels
    half = chips // 2
    steps = [(k, k + 1) for k in range(chips - 2, 1, -2) if k != half]
    steps = tuple(steps + [(half, 1), (half + 1, half + 1)])
    cores = [(d, d ^ 1) for d in range(devices)]
    crop = crop_flags.reshape(1, residues)
    limit = pltpu.CompilerParams(vmem_limit_bytes=48 * 1024 * 1024)
    anywhere = pl.BlockSpec(memory_space=pltpu.HBM)

    operands = (
        alignment,
        seq_flags.reshape(1, seqs),
        crop,
        norm_gain.reshape(1, -1),
        norm_bias.reshape(1, -1),
        left_weight.T,
        right_weight.T,
        left_bias.reshape(1, -1),
        right_bias.reshape(1, -1),
    )
    projected = pl.pallas_call(
        _project_kernel,
        out_shape=jax.ShapeDtypeStruct((2 * residues + 2 * FLAG_ROWS, lanes), BF16),
        in_specs=[anywhere] * len(operands),
        out_specs=_vmem(1)[0],
        scratch_shapes=[pltpu.VMEM(a.shape, a.dtype) for a in operands]
        + [pltpu.SemaphoreType.DMA((1,)), pltpu.SemaphoreType.DMA((len(operands) - 1,))],
        compiler_params=limit,
        name="project",
    )(*map(_stay, operands))
    other = lax.ppermute(projected, "row", cores)
    parcel = jax.ShapeDtypeStruct((residues + rows_chip + FLAG_ROWS, lanes), BF16)
    shared = jax.ShapeDtypeStruct((residues // 2 + rows_here + FLAG_ROWS, lanes), BF16)
    own, *parcels = pl.pallas_call(
        functools.partial(_pack_kernel, steps, rows_chip),
        out_shape=[parcel] * len(steps) + [shared],
        in_specs=_vmem(2),
        out_specs=_vmem(1 + len(steps)),
        compiler_params=limit,
        name="pack",
    )(projected, other)
    received, handed = [], []
    for (far, near), piece in zip(steps, parcels):
        pairs = [(2 * q + 1, 2 * (q ^ far) + 1) for q in range(chips)]
        pairs += [(2 * q, 2 * (q ^ near)) for q in range(chips)]
        received.append(lax.ppermute(piece, "row", pairs))
        handed.append(lax.ppermute(received[-1], "row", cores))

    columns = rows_here * width
    state = [
        jax.ShapeDtypeStruct((residues, columns), F32),
        jax.ShapeDtypeStruct((FLAG_ROWS, lanes), F32),
    ]
    weight, *spread = pl.pallas_call(
        functools.partial(_prepare_kernel, channels),
        out_shape=[
            jax.ShapeDtypeStruct((channels, channels * width), BF16),
            jax.ShapeDtypeStruct((residues, width), F32),
            jax.ShapeDtypeStruct((rows_here, width), F32),
            jax.ShapeDtypeStruct((1, width), F32),
        ],
        in_specs=_vmem(1) + [anywhere] * 2,
        out_specs=_vmem(4),
        scratch_shapes=[
            pltpu.VMEM(out_weight.shape, F32),
            pltpu.VMEM(crop.shape, crop.dtype),
            pltpu.SemaphoreType.DMA((2,)),
        ],
        compiler_params=limit,
        name="prepare",
    )(out_weight, _stay(crop), _stay(out_bias.reshape(1, -1)))

    early = [own] + received[:-1]
    carry = pl.pallas_call(
        functools.partial(_early_kernel, len(early)),
        out_shape=state,
        in_specs=_vmem(1 + len(early)),
        out_specs=_vmem(2),
        scratch_shapes=[pltpu.VMEM((len(early) * lanes, columns), BF16)],
        compiler_params=limit,
        name="early",
    )(weight, *early)
    late = handed[:-1]
    carry = pl.pallas_call(
        functools.partial(_late_kernel, len(late)),
        out_shape=state + [jax.ShapeDtypeStruct((lanes, columns), BF16)],
        in_specs=_vmem(4 + len(late)),
        out_specs=_vmem(3),
        scratch_shapes=[pltpu.VMEM((len(late) * lanes, columns), BF16)],
        compiler_params=limit,
        name="late",
    )(weight, *carry, received[-1], *late)
    tile = (rows_here, residues, width)
    return pl.pallas_call(
        _last_kernel,
        out_shape=jax.ShapeDtypeStruct(tile, BF16),
        in_specs=_vmem(8),
        out_specs=anywhere,
        scratch_shapes=[
            pltpu.VMEM(tile, BF16),
            pltpu.SemaphoreType.DMA((rows_here,)),
        ],
        compiler_params=limit,
        name="last",
    )(*spread, *carry, received[-1], handed[-1])


def solution(mesh):
    return jax.shard_map(
        per_device,
        mesh=mesh,
        in_specs=(
            P(("grp", "row"), None, None),
            P(("grp", "row")),
            P("grp"),
            P(),
            P(),
            P(),
            P(),
            P(),
            P(),
            P(),
            P(),
        ),
        out_specs=P(("grp", "row"), None, None),
        check_vma=False,
    )
```

```python
import functools

import jax
import jax.numpy as jnp
from jax import lax
from jax.experimental import pallas as pl
from jax.experimental.pallas import tpu as pltpu
from jax.sharding import PartitionSpec as P


F32 = jnp.float32
BF16 = jnp.bfloat16
FLAG_ROWS = 8


def _iota(shape, dim):
    return lax.broadcasted_iota(jnp.int32, shape, dim)


def _column(row):
    length = row.shape[1]
    square = (length, length)
    picked = jnp.where(
        _iota(square, 0) == _iota(square, 1), jnp.broadcast_to(row, square), 0.0
    )
    return jnp.sum(picked, axis=1, keepdims=True)


def _pick_lanes(row, pick):
    high = row.astype(BF16).astype(F32)
    middle = (row - high).astype(BF16).astype(F32)
    parts = jnp.concatenate([high, middle, row - high - middle, jnp.zeros_like(row)], axis=0)
    parts = jnp.concatenate([parts, jnp.zeros_like(parts)], axis=0).astype(BF16)
    return jnp.sum(jnp.dot(parts, pick, preferred_element_type=F32), axis=0, keepdims=True)


def _stay(array):
    return pltpu.with_memory_space_constraint(array, pltpu.HBM)


def _vmem(n):
    return [pl.BlockSpec(memory_space=pltpu.VMEM)] * n


def _project_kernel(
    x_hbm,
    flags_hbm,
    crop_hbm,
    gain_hbm,
    shift_hbm,
    wl_hbm,
    wr_hbm,
    lb_hbm,
    rb_hbm,
    out_ref,
    x_ref,
    flags_ref,
    crop_ref,
    gain_ref,
    shift_ref,
    wl_ref,
    wr_ref,
    lb_ref,
    rb_ref,
    x_sems,
    sems,
):
    seqs, residues, _ = x_ref.shape
    channels = wl_ref.shape[0]
    small = [
        pltpu.make_async_copy(src, dst, sems.at[n])
        for n, (src, dst) in enumerate(
            [
                (wr_hbm, wr_ref),
                (wl_hbm, wl_ref),
                (gain_hbm, gain_ref),
                (shift_hbm, shift_ref),
                (crop_hbm, crop_ref),
                (flags_hbm, flags_ref),
                (lb_hbm, lb_ref),
                (rb_hbm, rb_ref),
            ]
        )
    ]
    loads = [
        pltpu.make_async_copy(x_hbm, x_ref, x_sems.at[0])
    ]
    for copy in small + loads:
        copy.start()
    pair = 2 * seqs
    lanes = pair * channels
    first = (lax.axis_index("row") % 2) * seqs
    which = _iota((channels, lanes), 0)
    spread = _iota((channels, lanes), 1)
    pick_r = jnp.where(spread // pair == which, 1.0, 0.0).astype(BF16)
    pick_l = jnp.where(spread % channels == which, 1.0, 0.0).astype(BF16)
    lane = _iota((1, lanes), 1)
    seq_r = lane % pair - first
    seq_l = lane // channels - first
    for copy in small:
        copy.wait()
    turned = (((0,), (0,)), ((), ()))
    weights = jnp.concatenate(
        [
            lax.dot_general(ref[...], pick, turned, preferred_element_type=F32)
            for ref, pick in ((wr_ref, pick_r), (wl_ref, pick_l))
        ],
        axis=1,
    ).astype(BF16)
    weights = jnp.concatenate([weights, weights], axis=0)
    rb_rep = _pick_lanes(rb_ref[...], pick_r)
    lb_rep = _pick_lanes(lb_ref[...], pick_l)
    crop = _column(crop_ref[...].astype(F32))
    right = jnp.zeros((residues, lanes), F32)
    left = jnp.zeros((residues, lanes), F32)
    flag_r = jnp.zeros((1, lanes), F32)
    flag_l = jnp.zeros((1, lanes), F32)
    flag_row = jnp.zeros((1, lanes), F32)
    flags = flags_ref[...].astype(F32)
    for s in range(seqs):
        flag = jnp.broadcast_to(flags[:, s : s + 1], (1, lanes))
        flag_r = jnp.where(seq_r == s, flag, flag_r)
        flag_l = jnp.where(seq_l == s, flag, flag_l)
        flag_row = jnp.where(lane - first == s, flag, flag_row)
    for copy in loads:
        copy.wait()
    rows = []
    for s in range(seqs):
        values = x_ref[s].astype(F32)
        values = values - jnp.mean(values, axis=-1, keepdims=True)
        variance = jnp.mean(values * values, axis=-1, keepdims=True)
        normed = values * lax.rsqrt(variance + 1e-05) * gain_ref[...] + shift_ref[...]
        high = normed.astype(BF16)
        low = (normed - high.astype(F32)).astype(BF16)
        rows.append(jnp.concatenate([high, low], axis=1))
    product = jnp.dot(jnp.concatenate(rows, axis=0), weights, preferred_element_type=F32)
    for s in range(seqs):
        part = product[s * residues : (s + 1) * residues]
        right = jnp.where(seq_r == s, part[:, :lanes], right)
        left = jnp.where(seq_l == s, part[:, lanes:], left)
    out_ref[0:residues] = ((right + rb_rep) * (flag_r * crop)).astype(BF16)
    out_ref[residues : 2 * residues] = ((left + lb_rep) * (flag_l * crop)).astype(BF16)
    rows = _iota((2 * FLAG_ROWS, lanes), 0)
    out_ref[2 * residues :] = jnp.where(rows == 0, flag_row, 0.0).astype(BF16)


def _pack_kernel(steps, rows_chip, own_ref, other_ref, *out_refs):
    residues = own_ref.shape[0] // 2 - FLAG_ROWS
    half, rows_here = residues // 2, rows_chip // 2
    index = lax.axis_index("row")
    chip, core = index // 2, index % 2
    right = own_ref[0:residues] + other_ref[0:residues]
    flags = (own_ref[2 * residues :] + other_ref[2 * residues :]).astype(F32)[:FLAG_ROWS]
    for out_ref, (far, near) in zip(out_refs, ((0, 0),) + steps):
        target = chip ^ jnp.where(core == 1, far, near)
        start = pl.multiple_of(residues + target * rows_chip, rows_chip)
        slab = own_ref[pl.ds(start, rows_chip)] + other_ref[pl.ds(start, rows_chip)]
        slab = slab.astype(F32)
        if out_ref.shape[0] > residues:
            out_ref[0:residues] = right
            out_ref[residues:] = jnp.concatenate([slab, flags], axis=0).astype(BF16)
        else:
            out_ref[0:half] = jnp.where(core == 1, right[:half], right[half:])
            slab = jnp.where(core == 1, slab[rows_here:], slab[:rows_here])
            out_ref[half:] = jnp.concatenate([slab, flags], axis=0).astype(BF16)


def _spread(slabs, w_ref, targets):
    channels = w_ref.shape[0]
    rows_here, lanes = slabs[0].shape
    pair = lanes // channels
    width = w_ref.shape[1] // channels
    mine = _iota((pair, lanes), 1) // channels == _iota((pair, lanes), 0)
    rows = []
    for slab in slabs:
        for i in range(rows_here):
            rows.append(jnp.where(mine, jnp.broadcast_to(slab[i : i + 1], (pair, lanes)), 0.0))
    spread = jnp.concatenate(rows, axis=0).astype(BF16)
    for e in range(0, channels, 2):
        block = w_ref[:, e * width : (e + 2) * width]
        product = jnp.dot(
            spread, jnp.concatenate([block] * pair, axis=0), preferred_element_type=F32
        )
        for n, (a_ref, base) in enumerate(targets):
            for i in range(rows_here):
                at = (n * rows_here + i) * pair
                both = jnp.concatenate(
                    [product[at : at + pair, :width], product[at : at + pair, width:]], axis=0
                )
                a_ref[
                    base + e * pair : base + (e + 2) * pair, i * width : (i + 1) * width
                ] = both.astype(BF16)


def _slab(ref, residues):
    both = ref[residues : ref.shape[0] - FLAG_ROWS].astype(F32)
    half = both.shape[0] // 2
    return jnp.where(lax.axis_index("row") % 2 == 1, both[half:], both[:half])


def _contract(refs, a_ref, residues):
    lanes = refs[0].shape[1]
    total = None
    for n, ref in enumerate(refs):
        part = jnp.dot(
            ref[0:residues], a_ref[n * lanes : (n + 1) * lanes], preferred_element_type=F32
        )
        total = part if total is None else total + part
    return total


def _flags(refs):
    total = None
    for ref in refs:
        part = ref[ref.shape[0] - 2 * FLAG_ROWS :].astype(F32)[FLAG_ROWS:]
        total = part if total is None else total + part
    return total


def _prepare_kernel(
    channels, raw_ref, crop_hbm, bias_hbm, w_ref, column_ref, own_ref, bias_ref, wide_ref, crop_ref, sems
):
    loads = [
        pltpu.make_async_copy(src, dst, sems.at[n])
        for n, (src, dst) in enumerate([(crop_hbm, crop_ref), (bias_hbm, bias_ref)])
    ]
    for copy in loads:
        copy.start()
    width = raw_ref.shape[1]
    wide_ref[...] = raw_ref[...].astype(F32)
    for e in range(channels):
        block = wide_ref[pl.ds(e, channels, stride=channels), :]
        w_ref[:, e * width : (e + 1) * width] = block.astype(BF16)
    for copy in loads:
        copy.wait()
    crop = crop_ref[...].astype(F32)
    column_ref[...] = jnp.broadcast_to(_column(crop), column_ref.shape)
    rows_here = own_ref.shape[0]
    square = (rows_here, crop.shape[1])
    mine = _iota(square, 1) - lax.axis_index("row") * rows_here == _iota(square, 0)
    kept = jnp.where(mine, jnp.broadcast_to(crop, square), 0.0)
    own_ref[...] = jnp.broadcast_to(jnp.sum(kept, axis=1, keepdims=True), own_ref.shape)


def _early_kernel(count, w_ref, *refs):
    parcels, (sum_ref, flags_ref, a_ref) = refs[:count], refs[count:]
    residues, lanes = sum_ref.shape[0], parcels[0].shape[1]
    slabs = [_slab(ref, residues) for ref in parcels]
    _spread(slabs, w_ref, [(a_ref, n * lanes) for n in range(count)])
    sum_ref[...] = _contract(parcels, a_ref, residues)
    flags_ref[...] = _flags(parcels)


def _middle_kernel(count, w_ref, sum_in, flags_in, *refs):
    parcels, (sum_ref, flags_ref, a_ref) = refs[:count], refs[count:]
    residues, lanes = sum_ref.shape[0], parcels[0].shape[1]
    slabs = [_slab(ref, residues) for ref in parcels]
    _spread(slabs, w_ref, [(a_ref, n * lanes) for n in range(count)])
    sum_ref[...] = sum_in[...] + _contract(parcels, a_ref, residues)
    flags_ref[...] = flags_in[...] + _flags(parcels)


def _late_kernel(count, w_ref, sum_in, flags_in, shared_ref, *refs):
    parcels, (sum_ref, flags_ref, shared_a_ref, a_ref) = refs[:count], refs[count:]
    residues, lanes = sum_ref.shape[0], parcels[0].shape[1]
    slabs = [_slab(ref, residues) for ref in parcels]
    slabs.append(shared_ref[residues // 2 :].astype(F32)[:-FLAG_ROWS])
    targets = [(a_ref, n * lanes) for n in range(count)] + [(shared_a_ref, 0)]
    _spread(slabs, w_ref, targets)
    sum_ref[...] = sum_in[...] + _contract(parcels, a_ref, residues)
    flags_ref[...] = flags_in[...] + _flags(parcels + (shared_ref,))


def _last_kernel(
    column_ref,
    own_ref,
    bias_ref,
    sum_in,
    flags_in,
    a_ref,
    mine_ref,
    other_ref,
    out_hbm,
    out_ref,
    sems,
):
    rows_here, residues, width = out_ref.shape
    half = residues // 2
    core = lax.axis_index("row") % 2
    mine, other = mine_ref[0:half], other_ref[0:half]
    right = jnp.concatenate(
        [jnp.where(core == 1, mine, other), jnp.where(core == 1, other, mine)], axis=0
    )
    live = jnp.sum(jnp.sum(flags_in[...], axis=1, keepdims=True), axis=0, keepdims=True)
    inside = jnp.where(column_ref[...] > 0.0, 1.0 / jnp.maximum(live, 1.0), 1.0)
    stores = []
    group = 2 if rows_here % 2 == 0 else 1
    for first in range(0, rows_here, group):
        columns = slice(first * width, (first + group) * width)
        projected = sum_in[:, columns] + jnp.dot(
            right, a_ref[:, columns], preferred_element_type=F32
        )
        for i in range(first, first + group):
            scale = jnp.where(own_ref[i : i + 1] > 0.0, inside, 1.0)
            part = projected[:, (i - first) * width : (i - first + 1) * width]
            out_ref[i] = (part * scale + bias_ref[...]).astype(BF16)
            stores.append(pltpu.make_async_copy(out_ref.at[i], out_hbm.at[i], sems.at[i]))
            stores[-1].start()
    for copy in stores:
        copy.wait()


def per_device(
    alignment,
    seq_flags,
    crop_flags,
    norm_gain,
    norm_bias,
    left_weight,
    left_bias,
    right_weight,
    right_bias,
    out_weight,
    out_bias,
):
    seqs, residues, _ = alignment.shape
    channels = left_weight.shape[1]
    width = out_weight.shape[1]
    devices = lax.axis_size("row")
    rows_here = residues // devices
    rows_chip = 2 * rows_here
    chips = devices // 2
    lanes = 2 * seqs * channels
    half = chips // 2
    steps = [(k, k + 1) for k in range(chips - 2, 1, -2) if k != half]
    steps = tuple(steps + [(half, 1), (half + 1, half + 1)])
    cores = [(d, d ^ 1) for d in range(devices)]
    crop = crop_flags.reshape(1, residues)
    limit = pltpu.CompilerParams(vmem_limit_bytes=48 * 1024 * 1024)
    anywhere = pl.BlockSpec(memory_space=pltpu.HBM)

    operands = (
        alignment,
        seq_flags.reshape(1, seqs),
        crop,
        norm_gain.reshape(1, -1),
        norm_bias.reshape(1, -1),
        left_weight.T,
        right_weight.T,
        left_bias.reshape(1, -1),
        right_bias.reshape(1, -1),
    )
    projected = pl.pallas_call(
        _project_kernel,
        out_shape=jax.ShapeDtypeStruct((2 * residues + 2 * FLAG_ROWS, lanes), BF16),
        in_specs=[anywhere] * len(operands),
        out_specs=_vmem(1)[0],
        scratch_shapes=[pltpu.VMEM(a.shape, a.dtype) for a in operands]
        + [pltpu.SemaphoreType.DMA((1,)), pltpu.SemaphoreType.DMA((len(operands) - 1,))],
        compiler_params=limit,
        name="project",
    )(*map(_stay, operands))
    other = lax.ppermute(projected, "row", cores)
    parcel = jax.ShapeDtypeStruct((residues + rows_chip + FLAG_ROWS, lanes), BF16)
    shared = jax.ShapeDtypeStruct((residues // 2 + rows_here + FLAG_ROWS, lanes), BF16)
    own, *parcels = pl.pallas_call(
        functools.partial(_pack_kernel, steps, rows_chip),
        out_shape=[parcel] * len(steps) + [shared],
        in_specs=_vmem(2),
        out_specs=_vmem(1 + len(steps)),
        compiler_params=limit,
        name="pack",
    )(projected, other)
    received, handed = [], []
    for (far, near), piece in zip(steps, parcels):
        pairs = [(2 * q + 1, 2 * (q ^ far) + 1) for q in range(chips)]
        pairs += [(2 * q, 2 * (q ^ near)) for q in range(chips)]
        received.append(lax.ppermute(piece, "row", pairs))
        handed.append(lax.ppermute(received[-1], "row", cores))

    columns = rows_here * width
    state = [
        jax.ShapeDtypeStruct((residues, columns), F32),
        jax.ShapeDtypeStruct((FLAG_ROWS, lanes), F32),
    ]
    weight, *spread = pl.pallas_call(
        functools.partial(_prepare_kernel, channels),
        out_shape=[
            jax.ShapeDtypeStruct((channels, channels * width), BF16),
            jax.ShapeDtypeStruct((residues, width), F32),
            jax.ShapeDtypeStruct((rows_here, width), F32),
            jax.ShapeDtypeStruct((1, width), F32),
        ],
        in_specs=_vmem(1) + [anywhere] * 2,
        out_specs=_vmem(4),
        scratch_shapes=[
            pltpu.VMEM(out_weight.shape, F32),
            pltpu.VMEM(crop.shape, crop.dtype),
            pltpu.SemaphoreType.DMA((2,)),
        ],
        compiler_params=limit,
        name="prepare",
    )(out_weight, _stay(crop), _stay(out_bias.reshape(1, -1)))

    order = arrival(len(steps))
    early = [own] + [received[n] for n in order[:-3]]
    carry = pl.pallas_call(
        functools.partial(_early_kernel, len(early)),
        out_shape=state,
        in_specs=_vmem(1 + len(early)),
        out_specs=_vmem(2),
        scratch_shapes=[pltpu.VMEM((len(early) * lanes, columns), BF16)],
        compiler_params=limit,
        name="early",
    )(weight, *early)
    groups = {
        "second": [received[order[-3]]] + [handed[n] for n in order[:-3]],
        "middle": [received[order[-2]], handed[order[-3]]],
    }
    for group in groups.values():
        carry = pl.pallas_call(
            functools.partial(_middle_kernel, len(group)),
            out_shape=state,
            in_specs=_vmem(3 + len(group)),
            out_specs=_vmem(2),
            scratch_shapes=[pltpu.VMEM((len(group) * lanes, columns), BF16)],
            compiler_params=limit,
        )(weight, *carry, *group)
    carry = pl.pallas_call(
        functools.partial(_late_kernel, 1),
        out_shape=state + [jax.ShapeDtypeStruct((lanes, columns), BF16)],
        in_specs=_vmem(5),
        out_specs=_vmem(3),
        scratch_shapes=[pltpu.VMEM((lanes, columns), BF16)],
        compiler_params=limit,
        name="late",
    )(weight, *carry, received[-1], handed[order[-2]])
    tile = (rows_here, residues, width)
    return pl.pallas_call(
        _last_kernel,
        out_shape=jax.ShapeDtypeStruct(tile, BF16),
        in_specs=_vmem(8),
        out_specs=anywhere,
        scratch_shapes=[
            pltpu.VMEM(tile, BF16),
            pltpu.SemaphoreType.DMA((rows_here,)),
        ],
        compiler_params=limit,
        name="last",
    )(*spread, *carry, received[-1], handed[-1])


def arrival(count):
    return [0] + list(range(2, count - 1)) + [1, count - 1]


def solution(mesh):
    return jax.shard_map(
        per_device,
        mesh=mesh,
        in_specs=(
            P(("grp", "row"), None, None),
            P(("grp", "row")),
            P("grp"),
            P(),
            P(),
            P(),
            P(),
            P(),
            P(),
            P(),
            P(),
        ),
        out_specs=P(("grp", "row"), None, None),
        check_vma=False,
    )
```

```python
import functools

import jax
import jax.numpy as jnp
from jax import lax
from jax.experimental import pallas as pl
from jax.experimental.pallas import tpu as pltpu
from jax.sharding import PartitionSpec as P


F32 = jnp.float32
BF16 = jnp.bfloat16
FLAG_ROWS = 8


def _iota(shape, dim):
    return lax.broadcasted_iota(jnp.int32, shape, dim)


def _column(row):
    length = row.shape[1]
    square = (length, length)
    picked = jnp.where(
        _iota(square, 0) == _iota(square, 1), jnp.broadcast_to(row, square), 0.0
    )
    return jnp.sum(picked, axis=1, keepdims=True)


def _pick_lanes(row, pick):
    high = row.astype(BF16).astype(F32)
    middle = (row - high).astype(BF16).astype(F32)
    parts = jnp.concatenate([high, middle, row - high - middle, jnp.zeros_like(row)], axis=0)
    parts = jnp.concatenate([parts, jnp.zeros_like(parts)], axis=0).astype(BF16)
    return jnp.sum(jnp.dot(parts, pick, preferred_element_type=F32), axis=0, keepdims=True)


def _stay(array):
    return pltpu.with_memory_space_constraint(array, pltpu.HBM)


def _vmem(n):
    return [pl.BlockSpec(memory_space=pltpu.VMEM)] * n


def _project_kernel(
    x_hbm,
    flags_hbm,
    crop_hbm,
    gain_hbm,
    shift_hbm,
    wl_hbm,
    wr_hbm,
    lb_hbm,
    rb_hbm,
    out_ref,
    x_ref,
    flags_ref,
    crop_ref,
    gain_ref,
    shift_ref,
    wl_ref,
    wr_ref,
    lb_ref,
    rb_ref,
    x_sems,
    sems,
):
    seqs, residues, _ = x_ref.shape
    channels = wl_ref.shape[0]
    small = [
        pltpu.make_async_copy(src, dst, sems.at[n])
        for n, (src, dst) in enumerate(
            [
                (wr_hbm, wr_ref),
                (wl_hbm, wl_ref),
                (gain_hbm, gain_ref),
                (shift_hbm, shift_ref),
                (crop_hbm, crop_ref),
                (flags_hbm, flags_ref),
                (lb_hbm, lb_ref),
                (rb_hbm, rb_ref),
            ]
        )
    ]
    loads = [
        pltpu.make_async_copy(x_hbm, x_ref, x_sems.at[0])
    ]
    for copy in small + loads:
        copy.start()
    pair = 2 * seqs
    lanes = pair * channels
    first = (lax.axis_index("row") % 2) * seqs
    which = _iota((channels, lanes), 0)
    spread = _iota((channels, lanes), 1)
    pick_r = jnp.where(spread // pair == which, 1.0, 0.0).astype(BF16)
    pick_l = jnp.where(spread % channels == which, 1.0, 0.0).astype(BF16)
    lane = _iota((1, lanes), 1)
    seq_r = lane % pair - first
    seq_l = lane // channels - first
    for copy in small:
        copy.wait()
    turned = (((0,), (0,)), ((), ()))
    weights = jnp.concatenate(
        [
            lax.dot_general(ref[...], pick, turned, preferred_element_type=F32)
            for ref, pick in ((wr_ref, pick_r), (wl_ref, pick_l))
        ],
        axis=1,
    ).astype(BF16)
    weights = jnp.concatenate([weights, weights], axis=0)
    rb_rep = _pick_lanes(rb_ref[...], pick_r)
    lb_rep = _pick_lanes(lb_ref[...], pick_l)
    crop = _column(crop_ref[...].astype(F32))
    right = jnp.zeros((residues, lanes), F32)
    left = jnp.zeros((residues, lanes), F32)
    flag_r = jnp.zeros((1, lanes), F32)
    flag_l = jnp.zeros((1, lanes), F32)
    flag_row = jnp.zeros((1, lanes), F32)
    flags = flags_ref[...].astype(F32)
    for s in range(seqs):
        flag = jnp.broadcast_to(flags[:, s : s + 1], (1, lanes))
        flag_r = jnp.where(seq_r == s, flag, flag_r)
        flag_l = jnp.where(seq_l == s, flag, flag_l)
        flag_row = jnp.where(lane - first == s, flag, flag_row)
    for copy in loads:
        copy.wait()
    rows = []
    for s in range(seqs):
        values = x_ref[s].astype(F32)
        values = values - jnp.mean(values, axis=-1, keepdims=True)
        variance = jnp.mean(values * values, axis=-1, keepdims=True)
        normed = values * lax.rsqrt(variance + 1e-05) * gain_ref[...] + shift_ref[...]
        high = normed.astype(BF16)
        low = (normed - high.astype(F32)).astype(BF16)
        rows.append(jnp.concatenate([high, low], axis=1))
    product = jnp.dot(jnp.concatenate(rows, axis=0), weights, preferred_element_type=F32)
    for s in range(seqs):
        part = product[s * residues : (s + 1) * residues]
        right = jnp.where(seq_r == s, part[:, :lanes], right)
        left = jnp.where(seq_l == s, part[:, lanes:], left)
    out_ref[0:residues] = ((right + rb_rep) * (flag_r * crop)).astype(BF16)
    out_ref[residues : 2 * residues] = ((left + lb_rep) * (flag_l * crop)).astype(BF16)
    rows = _iota((2 * FLAG_ROWS, lanes), 0)
    out_ref[2 * residues :] = jnp.where(rows == 0, flag_row, 0.0).astype(BF16)


def _pack_kernel(steps, rows_chip, own_ref, other_ref, *out_refs):
    residues = own_ref.shape[0] // 2 - FLAG_ROWS
    half, rows_here = residues // 2, rows_chip // 2
    index = lax.axis_index("row")
    chip, core = index // 2, index % 2
    right = own_ref[0:residues] + other_ref[0:residues]
    flags = (own_ref[2 * residues :] + other_ref[2 * residues :]).astype(F32)[:FLAG_ROWS]
    for out_ref, (far, near) in zip(out_refs, ((0, 0),) + steps):
        target = chip ^ jnp.where(core == 1, far, near)
        start = pl.multiple_of(residues + target * rows_chip, rows_chip)
        slab = own_ref[pl.ds(start, rows_chip)] + other_ref[pl.ds(start, rows_chip)]
        slab = slab.astype(F32)
        if out_ref.shape[0] > residues:
            out_ref[0:residues] = right
            out_ref[residues:] = jnp.concatenate([slab, flags], axis=0).astype(BF16)
        else:
            out_ref[0:half] = jnp.where(core == 1, right[:half], right[half:])
            slab = jnp.where(core == 1, slab[rows_here:], slab[:rows_here])
            out_ref[half:] = jnp.concatenate([slab, flags], axis=0).astype(BF16)


def _spread(slabs, w_ref, targets):
    channels = w_ref.shape[0]
    rows_here, lanes = slabs[0].shape
    pair = lanes // channels
    width = w_ref.shape[1] // channels
    mine = _iota((pair, lanes), 1) // channels == _iota((pair, lanes), 0)
    rows = []
    for slab in slabs:
        for i in range(rows_here):
            rows.append(jnp.where(mine, jnp.broadcast_to(slab[i : i + 1], (pair, lanes)), 0.0))
    spread = jnp.concatenate(rows, axis=0).astype(BF16)
    for e in range(0, channels, 2):
        block = w_ref[:, e * width : (e + 2) * width]
        product = jnp.dot(
            spread, jnp.concatenate([block] * pair, axis=0), preferred_element_type=F32
        )
        for n, (a_ref, base) in enumerate(targets):
            for i in range(rows_here):
                at = (n * rows_here + i) * pair
                both = jnp.concatenate(
                    [product[at : at + pair, :width], product[at : at + pair, width:]], axis=0
                )
                a_ref[
                    base + e * pair : base + (e + 2) * pair, i * width : (i + 1) * width
                ] = both.astype(BF16)


def _slab(ref, residues):
    both = ref[residues : ref.shape[0] - FLAG_ROWS].astype(F32)
    half = both.shape[0] // 2
    return jnp.where(lax.axis_index("row") % 2 == 1, both[half:], both[:half])


def _contract(refs, a_ref, residues):
    lanes = refs[0].shape[1]
    total = None
    for n, ref in enumerate(refs):
        part = jnp.dot(
            ref[0:residues], a_ref[n * lanes : (n + 1) * lanes], preferred_element_type=F32
        )
        total = part if total is None else total + part
    return total


def _flags(refs):
    total = None
    for ref in refs:
        part = ref[ref.shape[0] - 2 * FLAG_ROWS :].astype(F32)[FLAG_ROWS:]
        total = part if total is None else total + part
    return total


def _prepare_kernel(
    channels, raw_ref, crop_hbm, bias_hbm, w_ref, column_ref, own_ref, bias_ref, wide_ref, crop_ref, sems
):
    loads = [
        pltpu.make_async_copy(src, dst, sems.at[n])
        for n, (src, dst) in enumerate([(crop_hbm, crop_ref), (bias_hbm, bias_ref)])
    ]
    for copy in loads:
        copy.start()
    width = raw_ref.shape[1]
    wide_ref[...] = raw_ref[...].astype(F32)
    for e in range(channels):
        block = wide_ref[pl.ds(e, channels, stride=channels), :]
        w_ref[:, e * width : (e + 1) * width] = block.astype(BF16)
    for copy in loads:
        copy.wait()
    crop = crop_ref[...].astype(F32)
    column_ref[...] = jnp.broadcast_to(_column(crop), column_ref.shape)
    rows_here = own_ref.shape[0]
    square = (rows_here, crop.shape[1])
    mine = _iota(square, 1) - lax.axis_index("row") * rows_here == _iota(square, 0)
    kept = jnp.where(mine, jnp.broadcast_to(crop, square), 0.0)
    own_ref[...] = jnp.broadcast_to(jnp.sum(kept, axis=1, keepdims=True), own_ref.shape)


def _early_kernel(count, w_ref, *refs):
    parcels, (sum_ref, flags_ref, a_ref) = refs[:count], refs[count:]
    residues, lanes = sum_ref.shape[0], parcels[0].shape[1]
    slabs = [_slab(ref, residues) for ref in parcels]
    _spread(slabs, w_ref, [(a_ref, n * lanes) for n in range(count)])
    sum_ref[...] = _contract(parcels, a_ref, residues)
    flags_ref[...] = _flags(parcels)


def _middle_kernel(count, w_ref, sum_in, flags_in, *refs):
    parcels, (sum_ref, flags_ref, a_ref) = refs[:count], refs[count:]
    residues, lanes = sum_ref.shape[0], parcels[0].shape[1]
    slabs = [_slab(ref, residues) for ref in parcels]
    _spread(slabs, w_ref, [(a_ref, n * lanes) for n in range(count)])
    sum_ref[...] = sum_in[...] + _contract(parcels, a_ref, residues)
    flags_ref[...] = flags_in[...] + _flags(parcels)


def _finish(total, refs, other, live, out_ref, out_hbm, sems):
    column_ref, own_ref, bias_ref = refs
    rows_here, half, width = out_ref.shape
    upper = (lax.axis_index("row") % 2 == 1) != other
    column = jnp.where(upper, column_ref[0:half], column_ref[half:])
    offset = pl.multiple_of(jnp.where(upper, 0, half), half)
    inside = jnp.where(column > 0.0, 1.0 / jnp.maximum(live, 1.0), 1.0)
    stores = []
    for i in range(rows_here):
        scale = jnp.where(own_ref[i : i + 1] > 0.0, inside, 1.0)
        part = total[:, i * width : (i + 1) * width]
        out_ref[i] = (part * scale + bias_ref[...]).astype(BF16)
        stores.append(
            pltpu.make_async_copy(out_ref.at[i], out_hbm.at[i, pl.ds(offset, half)], sems.at[i])
        )
        stores[-1].start()
    for copy in stores:
        copy.wait()


def _total(flags):
    return jnp.sum(jnp.sum(flags, axis=1, keepdims=True), axis=0, keepdims=True)


def _late_kernel(
    w_ref,
    column_ref,
    own_ref,
    bias_ref,
    sum_in,
    flags_in,
    shared_ref,
    parcel_ref,
    rest_ref,
    flags_ref,
    shared_a_ref,
    out_hbm,
    a_ref,
    out_ref,
    sems,
):
    residues = sum_in.shape[0]
    half = residues // 2
    north = lax.axis_index("row") % 2 == 1
    slabs = [_slab(parcel_ref, residues), shared_ref[half:].astype(F32)[:-FLAG_ROWS]]
    _spread(slabs, w_ref, [(a_ref, 0), (shared_a_ref, 0)])
    total = sum_in[...] + _contract((parcel_ref,), a_ref, residues)
    rest_ref[...] = jnp.where(north, total[half:], total[:half])
    mine = jnp.where(north, total[:half], total[half:])
    mine = mine + jnp.dot(shared_ref[0:half], shared_a_ref[...], preferred_element_type=F32)
    flags = flags_in[...] + _flags((parcel_ref, shared_ref))
    flags_ref[...] = flags
    refs = (column_ref, own_ref, bias_ref)
    _finish(mine, refs, False, _total(flags), out_ref, out_hbm, sems)


def _last_kernel(
    column_ref,
    own_ref,
    bias_ref,
    rest_ref,
    flags_ref,
    a_ref,
    other_ref,
    begun_hbm,
    out_hbm,
    out_ref,
    sems,
):
    half = rest_ref.shape[0]
    total = rest_ref[...] + jnp.dot(
        other_ref[0:half], a_ref[...], preferred_element_type=F32
    )
    refs = (column_ref, own_ref, bias_ref)
    _finish(total, refs, True, _total(flags_ref[...]), out_ref, out_hbm, sems)


def per_device(
    alignment,
    seq_flags,
    crop_flags,
    norm_gain,
    norm_bias,
    left_weight,
    left_bias,
    right_weight,
    right_bias,
    out_weight,
    out_bias,
):
    seqs, residues, _ = alignment.shape
    channels = left_weight.shape[1]
    width = out_weight.shape[1]
    devices = lax.axis_size("row")
    rows_here = residues // devices
    rows_chip = 2 * rows_here
    chips = devices // 2
    lanes = 2 * seqs * channels
    half = chips // 2
    steps = [(k, k + 1) for k in range(chips - 2, 1, -2) if k != half]
    steps = tuple(steps + [(half, 1), (half + 1, half + 1)])
    cores = [(d, d ^ 1) for d in range(devices)]
    crop = crop_flags.reshape(1, residues)
    limit = pltpu.CompilerParams(vmem_limit_bytes=48 * 1024 * 1024)
    anywhere = pl.BlockSpec(memory_space=pltpu.HBM)

    operands = (
        alignment,
        seq_flags.reshape(1, seqs),
        crop,
        norm_gain.reshape(1, -1),
        norm_bias.reshape(1, -1),
        left_weight.T,
        right_weight.T,
        left_bias.reshape(1, -1),
        right_bias.reshape(1, -1),
    )
    projected = pl.pallas_call(
        _project_kernel,
        out_shape=jax.ShapeDtypeStruct((2 * residues + 2 * FLAG_ROWS, lanes), BF16),
        in_specs=[anywhere] * len(operands),
        out_specs=_vmem(1)[0],
        scratch_shapes=[pltpu.VMEM(a.shape, a.dtype) for a in operands]
        + [pltpu.SemaphoreType.DMA((1,)), pltpu.SemaphoreType.DMA((len(operands) - 1,))],
        compiler_params=limit,
        name="project",
    )(*map(_stay, operands))
    other = lax.ppermute(projected, "row", cores)
    parcel = jax.ShapeDtypeStruct((residues + rows_chip + FLAG_ROWS, lanes), BF16)
    shared = jax.ShapeDtypeStruct((residues // 2 + rows_here + FLAG_ROWS, lanes), BF16)
    own, *parcels = pl.pallas_call(
        functools.partial(_pack_kernel, steps, rows_chip),
        out_shape=[parcel] * len(steps) + [shared],
        in_specs=_vmem(2),
        out_specs=_vmem(1 + len(steps)),
        compiler_params=limit,
        name="pack",
    )(projected, other)
    received, handed = [], []
    for (far, near), piece in zip(steps, parcels):
        pairs = [(2 * q + 1, 2 * (q ^ far) + 1) for q in range(chips)]
        pairs += [(2 * q, 2 * (q ^ near)) for q in range(chips)]
        received.append(lax.ppermute(piece, "row", pairs))
        handed.append(lax.ppermute(received[-1], "row", cores))

    columns = rows_here * width
    state = [
        jax.ShapeDtypeStruct((residues, columns), F32),
        jax.ShapeDtypeStruct((FLAG_ROWS, lanes), F32),
    ]
    weight, *spread = pl.pallas_call(
        functools.partial(_prepare_kernel, channels),
        out_shape=[
            jax.ShapeDtypeStruct((channels, channels * width), BF16),
            jax.ShapeDtypeStruct((residues, width), F32),
            jax.ShapeDtypeStruct((rows_here, width), F32),
            jax.ShapeDtypeStruct((1, width), F32),
        ],
        in_specs=_vmem(1) + [anywhere] * 2,
        out_specs=_vmem(4),
        scratch_shapes=[
            pltpu.VMEM(out_weight.shape, F32),
            pltpu.VMEM(crop.shape, crop.dtype),
            pltpu.SemaphoreType.DMA((2,)),
        ],
        compiler_params=limit,
        name="prepare",
    )(out_weight, _stay(crop), _stay(out_bias.reshape(1, -1)))

    order = arrival(len(steps))
    early = [own] + [received[n] for n in order[:-3]]
    carry = pl.pallas_call(
        functools.partial(_early_kernel, len(early)),
        out_shape=state,
        in_specs=_vmem(1 + len(early)),
        out_specs=_vmem(2),
        scratch_shapes=[pltpu.VMEM((len(early) * lanes, columns), BF16)],
        compiler_params=limit,
        name="early",
    )(weight, *early)
    groups = {
        "second": [received[order[-3]]] + [handed[n] for n in order[:-3]],
        "middle": [received[order[-2]], handed[order[-3]]],
    }
    for group in groups.values():
        carry = pl.pallas_call(
            functools.partial(_middle_kernel, len(group)),
            out_shape=state,
            in_specs=_vmem(3 + len(group)),
            out_specs=_vmem(2),
            scratch_shapes=[pltpu.VMEM((len(group) * lanes, columns), BF16)],
            compiler_params=limit,
        )(weight, *carry, *group)
    tile = jax.ShapeDtypeStruct((rows_here, residues, width), BF16)
    stage = [
        pltpu.VMEM((rows_here, residues // 2, width), BF16),
        pltpu.SemaphoreType.DMA((rows_here,)),
    ]
    *carry, begun = pl.pallas_call(
        _late_kernel,
        out_shape=[
            jax.ShapeDtypeStruct((residues // 2, columns), F32),
            state[1],
            jax.ShapeDtypeStruct((lanes, columns), BF16),
            tile,
        ],
        in_specs=_vmem(8),
        out_specs=_vmem(3) + [anywhere],
        scratch_shapes=[pltpu.VMEM((lanes, columns), BF16)] + stage,
        compiler_params=limit,
        name="late",
    )(weight, *spread, *carry, received[-1], handed[order[-2]])
    return pl.pallas_call(
        _last_kernel,
        out_shape=tile,
        in_specs=_vmem(7) + [anywhere],
        out_specs=anywhere,
        scratch_shapes=stage,
        input_output_aliases={7: 0},
        compiler_params=limit,
        name="last",
    )(*spread, *carry, handed[-1], begun)


def arrival(count):
    return [0] + list(range(2, count - 1)) + [1, count - 1]


def solution(mesh):
    return jax.shard_map(
        per_device,
        mesh=mesh,
        in_specs=(
            P(("grp", "row"), None, None),
            P(("grp", "row")),
            P("grp"),
            P(),
            P(),
            P(),
            P(),
            P(),
            P(),
            P(),
            P(),
        ),
        out_specs=P(("grp", "row"), None, None),
        check_vma=False,
    )
```
